8 devices in a mesh: dp: 1 (over z), tp: 8 (over x, y, core).
Axes of the slice: x: 2, y: 2, z: 1, core: 2. Of those that a mesh axis runs over, the one named last changes fastest.
Arguments:
- x: bfloat16 [1, 1024, 8192], P('dp', 'tp')
- dy: bfloat16 [1, 1024, 8192], P('dp', 'tp')
- wq: bfloat16 [8192, 8192], P(None, 'tp')
- wk: bfloat16 [8192, 1024], P(None, 'tp')
- wv: bfloat16 [8192, 1024], P(None, 'tp')
- wo: bfloat16 [8192, 8192], P('tp')
- w_gate: bfloat16 [8192, 28672], P(None, 'tp')
- w_up: bfloat16 [8192, 28672], P(None, 'tp')
- w_down: bfloat16 [28672, 8192], P('tp')
Outputs:
- output 1: bfloat16 [1, 1024, 8192], P('dp', 'tp')
- output 2: bfloat16 [8192, 8192], P('dp', 'tp')
- output 3: bfloat16 [8192, 1024], P('dp', 'tp')
- output 4: bfloat16 [8192, 1024], P('dp', 'tp')
- output 5: bfloat16 [8192, 8192], P(('dp', 'tp'))
- output 6: bfloat16 [8192, 28672], P('dp', 'tp')
- output 7: bfloat16 [8192, 28672], P('dp', 'tp')
- output 8: bfloat16 [28672, 8192], P(('dp', 'tp'))
All inputs are finite; a program needn't handle non-finite values.
Results may differ from the reference program's by a relative error of at most 0.024.
Values are sent between devices in bfloat16 or wider.
A program may use at most 2 GiB of HBM per device.

```python
import jax
import jax.numpy as jnp
from jax import lax

SEQUENCES = 1
TOKENS = 1024
D = 8192
HEADS = 64
KV_HEADS = 8
HEAD = 128
FF = 28672
THETA = 10000
NAMES = ("wq", "wk", "wv", "wo", "w_gate", "w_up", "w_down")
SHAPES = {
    "wq": (D, HEADS * HEAD),
    "wk": (D, KV_HEADS * HEAD),
    "wv": (D, KV_HEADS * HEAD),
    "wo": (HEADS * HEAD, D),
    "w_gate": (D, FF),
    "w_up": (D, FF),
    "w_down": (FF, D),
}


def bump(key, n, height):
    away = (jnp.arange(n, dtype=jnp.int32) - jax.random.randint(key, (), 0, n, jnp.int32)) % n
    return jnp.where(away < n // 8, height, 1.0)


def together(key, own, strength):
    shared = jax.random.normal(key, own.shape[1:], jnp.float32)
    return (own + strength * shared) * lax.rsqrt(1 + strength * strength)


def setup_inputs(seed: int = 0, part: int = 0) -> dict:
    kx, kdy, ka, kb, kz, kf, kh, kl, *kw = jax.random.split(jax.random.key(seed), 8 + len(NAMES))
    kx, kdy, ka, kb = (jax.random.fold_in(k, part) for k in (kx, kdy, ka, kb))
    shape = (SEQUENCES, TOKENS, D)
    much_x, much_dy = jax.random.uniform(kz, (2,), jnp.float32, 0.0, 1.0)
    loud = 2.0 ** jax.random.uniform(jax.random.fold_in(kz, 1), (), jnp.float32, -1.0, 2.0)
    halves = 2.0 ** jax.random.uniform(kl, (2,), jnp.float32, -1.0, 1.0)
    times = {"wq": 1.0, "wk": 1.0, "wv": 2.0, "wo": halves[0], "w_gate": 1.0, "w_up": bump(kh, FF, 4.0), "w_down": halves[1]}
    x = together(ka, jax.random.normal(kx, shape, jnp.float32), much_x) * bump(kf, D, 4.0)
    dy = together(kb, jax.random.normal(kdy, shape, jnp.float32), much_dy)
    drawn = {"x": x.astype(jnp.bfloat16), "dy": (loud * dy * (SEQUENCES * TOKENS) ** -0.5).astype(jnp.bfloat16)}
    for key, name in zip(kw, NAMES, strict=True):
        drawn[name] = (jax.random.normal(key, SHAPES[name], jnp.float32) * SHAPES[name][0] ** -0.5 * times[name]).astype(jnp.bfloat16)
    return drawn


def matmul(a, w):
    return jnp.dot(a, w, preferred_element_type=jnp.float32).astype(jnp.bfloat16)


def normed(h):
    wide = h.astype(jnp.float32)
    scale = lax.rsqrt(jnp.mean(wide**2, -1, keepdims=True) + 1e-6)
    return (wide * scale).astype(jnp.bfloat16)


def turned(t, theta):
    half = t.shape[-1] // 2
    angle = jnp.arange(t.shape[0], dtype=jnp.float32)[:, None] * theta ** (-jnp.arange(half, dtype=jnp.float32) / half)
    cos, sin = jnp.cos(angle)[:, None], jnp.sin(angle)[:, None]
    a, b = t[..., :half].astype(jnp.float32), t[..., half:].astype(jnp.float32)
    return jnp.concatenate([a * cos - b * sin, b * cos + a * sin], -1).astype(jnp.bfloat16)


def seen_by(q, k, v):
    tokens, kv = q.shape[0], k.shape[1]
    q = q.reshape(tokens, kv, -1, q.shape[-1])
    scores = jnp.einsum("tgsd,ugd->gstu", q.astype(jnp.float32), k.astype(jnp.float32)) * q.shape[-1] ** -0.5
    place = jnp.arange(tokens)
    weights = jax.nn.softmax(jnp.where(place[:, None] >= place, scores, -jnp.inf), -1).astype(jnp.bfloat16)
    return jnp.einsum("gstu,ugd->tgsd", weights.astype(jnp.float32), v.astype(jnp.float32)).astype(jnp.bfloat16).reshape(tokens, -1)


def layer(h, w):
    a = normed(h)
    q, k = (turned(matmul(a, w[name]).reshape(h.shape[0], -1, HEAD), THETA) for name in ("wq", "wk"))
    h = h + matmul(seen_by(q, k, matmul(a, w["wv"]).reshape(h.shape[0], -1, HEAD)), w["wo"])
    b = normed(h)
    gate = jnp.dot(b, w["w_gate"], preferred_element_type=jnp.float32)
    up = jnp.dot(b, w["w_up"], preferred_element_type=jnp.float32)
    return h + matmul((jax.nn.silu(gate) * up).astype(jnp.bfloat16), w["w_down"])


def reference(x, dy, wq, wk, wv, wo, w_gate, w_up, w_down):
    weights = dict(zip(NAMES, (wq, wk, wv, wo, w_gate, w_up, w_down), strict=True))

    def take(so_far, sequence):
        h, by_y = sequence
        _, back = jax.vjp(lambda w, h: layer(h, w), weights, h)
        by_weights, by_h = back(by_y)
        return jax.tree.map(lambda total, term: total + term.astype(jnp.float32), so_far, by_weights), by_h

    none_yet = {name: jnp.zeros(w.shape, jnp.float32) for name, w in weights.items()}
    by_weights, by_x = lax.scan(take, none_yet, (x, dy))
    return (by_x, *(by_weights[name].astype(jnp.bfloat16) for name in NAMES))
```

```python
import functools

import jax
import jax.numpy as jnp
import numpy as np
from jax import lax
from jax.experimental import pallas as pl
from jax.experimental.pallas import tpu as pltpu
from jax.sharding import PartitionSpec as P

HEAD = 128
THETA = 10000
SHARD = 128
PART = SHARD // 2
PAIR = 2 * SHARD
MESH = pl.DeviceIdType.MESH
DMA = pltpu.SemaphoreType.DMA
F32, BF16 = jnp.float32, jnp.bfloat16
ANY = pl.BlockSpec(memory_space=pl.ANY)
EPS = 1e-6
MIB = 2**20
BOTH, AWAY, QUARTERS = range(2), range(1, 4), 4
STILL = lambda *_: (0, 0)
NEG = -1e30
HIDDEN = 2 * NEG
LOG2E = 1.4426950408889634


def _contract(ca, cb):
    return lambda a, b: lax.dot_general(a, b, (((ca,), (cb,)), ((), ())), preferred_element_type=F32)


nn, nt, tt = _contract(1, 0), _contract(1, 1), _contract(0, 0)


def _params(vmem, cid=None, **more):
    if cid is not None:
        more |= {"collective_id": cid, "has_side_effects": True}
    return pltpu.CompilerParams(vmem_limit_bytes=vmem * MIB, **more)


def _down(rows, columns):
    return pl.BlockSpec((rows, columns), lambda i: (i, 0))


def _along(rows, columns):
    return pl.BlockSpec((rows, columns), lambda i: (0, i))


def _cost(flops, nbytes, exps=0):
    return pl.CostEstimate(flops=flops, transcendentals=exps, bytes_accessed=nbytes)


def _hidden(first_key, first_query, bk, bq):
    keys = lax.broadcasted_iota(jnp.int32, (bk, bq), 0) + first_key
    return keys > lax.broadcasted_iota(jnp.int32, (bk, bq), 1) + first_query


def _head(n):
    return slice(n * HEAD, (n + 1) * HEAD)


def _blocks(block, iq, n):
    lax.fori_loop(0, iq * n, lambda j, _: block(j, False), None)
    lax.fori_loop(iq * n, (iq + 1) * n, lambda j, _: block(j, True), None)


def _attend(q, k, v, o, lse, top_s, mix_s, iq, bk):
    bq, heads = top_s.shape[1], top_s.shape[0]
    scale = HEAD**-0.5
    e = scale * LOG2E
    rows = pl.ds(pl.multiple_of(iq * bq, bq), bq)
    top_s[...] = jnp.full(top_s.shape, NEG, F32)
    mix_s[...] = jnp.zeros(mix_s.shape, F32)
    ones = jnp.ones((mix_s.shape[1] - HEAD, bk), BF16)

    def block(j, masked):
        here = pl.ds(pl.multiple_of(j * bk, bk), bk)
        scores = [nt(k[here, :], q[rows, _head(n)]) for n in range(heads)]
        hide = _hidden(j * bk, iq * bq, bk, bq) if masked else None
        weights, keeps = [], []
        for n, s in enumerate(scores):
            if masked:
                s = jnp.where(hide, HIDDEN, s)
            old = top_s[n : n + 1, :]
            top = jnp.maximum(old, s.max(axis=0, keepdims=True))
            top_s[n : n + 1, :] = top
            weights.append(jnp.exp2((s - top) * e).astype(BF16))
            keeps.append(jnp.exp2((old - top) * e))
        values = jnp.concatenate([v[here, :].T, ones], axis=0)
        for n in range(heads):
            mix_s[n] = mix_s[n] * keeps[n] + nn(values, weights[n])

    _blocks(block, iq, bq // bk)
    for n in range(heads):
        total = mix_s[n, HEAD : HEAD + 1, :]
        o[rows, _head(n)] = (mix_s[n, :HEAD, :] * (1 / total)).T.astype(BF16)
        lse[n : n + 1, rows] = top_s[n : n + 1, :] * scale + jnp.log(total)


def _unturned(t, c, n):
    t = t.astype(BF16).astype(F32)
    return (t * c - pltpu.roll(t, HEAD // 2, 1) * n).astype(BF16)


def _attend_bwd(q_ref, k_ref, v_ref, do_ref, o_ref, lse_ref, cos_ref, sin_ref, cosk_ref, sink_ref, dq_ref, dkv_ref, dq_s, dk_s, dv_s, delta_s, *, bk):
    bq, heads = q_ref.shape[0], q_ref.shape[1] // HEAD
    iq = pl.program_id(0)
    scale = HEAD**-0.5
    e = scale * LOG2E

    @pl.when(iq == 0)
    def _():
        dk_s[...] = jnp.zeros_like(dk_s)
        dv_s[...] = jnp.zeros_like(dv_s)

    dq_s[...] = jnp.zeros_like(dq_s)
    for n in range(heads):
        both = do_ref[:, _head(n)].astype(F32) * o_ref[:, _head(n)].astype(F32)
        delta_s[n : n + 1, :] = both.T.sum(axis=0, keepdims=True)

    def block(j, masked):
        here = pl.ds(pl.multiple_of(j * bk, bk), bk)
        scores = [nt(k_ref[here, :], q_ref[:, _head(n)]) for n in range(heads)]
        dps = [nt(v_ref[here, :], do_ref[:, _head(n)]) for n in range(heads)]
        hide = _hidden(j * bk, iq * bq, bk, bq) if masked else None
        for n in range(heads):
            p = jnp.exp2(scores[n] * e - lse_ref[n : n + 1, :] * LOG2E)
            if masked:
                p = jnp.where(hide, 0.0, p)
            ds = (p * (dps[n] - delta_s[n : n + 1, :])).astype(BF16)
            dv_s[here, :] += nn(p.astype(BF16), do_ref[:, _head(n)])
            dk_s[here, :] += nn(ds, q_ref[:, _head(n)])
            dq_s[n] += nn(k_ref[here, :].T, ds)

    _blocks(block, iq, bq // bk)
    for n in range(heads):
        dq_ref[:, _head(n)] = _unturned((dq_s[n] * scale).T, cos_ref[...], sin_ref[...])

    @pl.when(iq == pl.num_programs(0) - 1)
    def _():
        dkv_ref[:, :HEAD] = _unturned(dk_s[...] * scale, cosk_ref[...], sink_ref[...])
        dkv_ref[:, HEAD:] = dv_s[...].astype(BF16)


def attend_bwd(q, k, v, d_o, o, lse, cos, sin, bq=256, bk=256):
    tokens, d = q.shape
    heads = d // HEAD
    rows = _down(bq, d)
    some, every = _down(bq, HEAD), pl.BlockSpec((tokens, HEAD), STILL)
    return pl.pallas_call(
        functools.partial(_attend_bwd, bk=bk),
        grid=(tokens // bq,),
        in_specs=[rows, every, every, rows, rows, _along(heads, bq), some, some, every, every],
        out_specs=[rows, pl.BlockSpec((tokens, 2 * HEAD), STILL)],
        out_shape=[jax.ShapeDtypeStruct((tokens, d), BF16), jax.ShapeDtypeStruct((tokens, 2 * HEAD), BF16)],
        scratch_shapes=[pltpu.VMEM((heads, HEAD, bq), F32), pltpu.VMEM((tokens, HEAD), F32), pltpu.VMEM((tokens, HEAD), F32), pltpu.VMEM((heads, bq), F32)],
        compiler_params=_params(56),
        cost_estimate=_cost(10 * tokens * tokens * d, 10 * tokens * d, tokens * tokens * heads),
        name="attend_bwd",
    )(q, k, v, d_o, o, lse, cos, sin, cos, sin)


def _flip(c):
    return c + (c // 2) * (1 - 2 * (c % 2))


def _place():
    me = lax.axis_index("tp")
    core, pos = me % 2, _flip(me // 2)
    turn = 1 - 2 * core
    at = lambda k, c: _flip((pos + turn * k + 8) % 4) * 2 + c
    return core, at, me + turn, at(1, core), at(-1, core)


def _owner(at, core, s, side):
    return at(-s if side == 0 else s, core if side == 0 else 1 - core)


def _greet(devices):
    barrier = pltpu.get_barrier_semaphore()
    for d in devices:
        pl.semaphore_signal(barrier, inc=1, device_id={"tp": d}, device_id_type=MESH)
    pl.semaphore_wait(barrier, len(devices))


def _send(src, dst, ssem, rsem, dev):
    return pltpu.make_async_remote_copy(src_ref=src, dst_ref=dst, send_sem=ssem, recv_sem=rsem, device_id={"tp": dev}, device_id_type=MESH)


def _place_of(s, half, side):
    return ((s * 2 + half) * 2 + side) * PART


class _Gather:
    def __init__(self, ref, sems, nxt, partner):
        self.ref, self.sems, self.nxt, self.partner = ref, sems, nxt, partner

    def part(self, s, half, side):
        return self.ref.at[pl.ds(pl.multiple_of(_place_of(s, half, side), PART), PART)]

    def ring(self, s, half, src=None):
        rs, rr, _, _ = self.sems
        return _send(self.part(s, half, 0) if src is None else src, self.part(s + 1, half, 0), rs.at[s, half], rr.at[s + 1, half], self.nxt)

    def across(self, s, half, src=None):
        _, _, xs, xr = self.sems
        return _send(self.part(s, half, 0) if src is None else src, self.part(s, half, 1), xs.at[s, half], xr.at[s, half], self.partner)


GATHER_SEMS = [DMA((4, 2))] * 4


def _norm_rows(src, dst, at_row, rows, step=16):
    def body(i, _):
        r = pl.multiple_of(i * step, step)
        wide = src[pl.ds(r, step), :].astype(F32)
        scale = lax.rsqrt(jnp.mean(wide * wide, -1, keepdims=True) + EPS)
        dst[pl.ds(pl.multiple_of(at_row(r), step), step), :] = (wide * scale).astype(BF16)

    lax.fori_loop(rows[0] // step, rows[1] // step, body, None)


def _qkv(x, dy, wq, wk, wv, cos, sin, q_out, k_out, v_out, a_out, y_out, o, lse, xb, yb, A, W, cosb, sinb, O, top_s, mix_s,
         rs, rr, xs, xr, ys, yr, zs, zr, lsem, osem, asem, bk):
    core, at, partner, nxt, prv = _place()
    gather = _Gather(A, (rs, rr, xs, xr), nxt, partner)
    gather_y = _Gather(y_out, (ys, yr, zs, zr), nxt, partner)
    hq = wq.shape[1]
    hk = wk.shape[1]
    cuts = (pl.ds(0, hq), pl.ds(hq, hk), pl.ds(hq + hk, hk))
    moves = ((x, xb), (cos, cosb), (sin, sinb), *((w, W.at[:, c]) for w, c in zip((wq, wk, wv), cuts)), (dy, yb))
    loads = [pltpu.make_async_copy(a, b, lsem.at[i]) for i, (a, b) in enumerate(moves)]
    for c in loads:
        c.start()
    _greet((partner, nxt, prv))
    loads[0].wait()
    own = [yb.at[pl.ds(half * PART, PART)] for half in BOTH]
    keep_y = [pltpu.make_async_copy(own[half], gather_y.part(0, half, 0), asem.at[QUARTERS, half, 0]) for half in BOTH]
    for half in BOTH:
        _norm_rows(xb, A, lambda r: r + half * PART, (half * PART, half * PART + PART))
        gather.ring(0, half).start()
        gather.across(0, half).start()
    for c in loads[1:]:
        c.wait()
    for half in BOTH:
        keep_y[half].start()
        gather_y.across(0, half, own[half]).start()

    def there(s, half, side):
        return pl.ds(pl.multiple_of(_owner(at, core, s, side) * SHARD + half * PART, PART), PART)

    def keep(s, half, side):
        return pltpu.make_async_copy(gather.part(s, half, side), a_out.at[there(s, half, side)], asem.at[s, half, side])

    def unit(u, _):
        s, half = u // 2, u % 2

        @pl.when(s > 0)
        def _():
            gather.ring(s - 1, half).wait_recv()

            @pl.when(s < AWAY[-1])
            def _():
                gather.ring(s, half).start()

            gather.across(s, half).start()

        @pl.when(s == AWAY[-1])
        def _():
            gather_y.ring(0, half, yb.at[pl.ds(pl.multiple_of(half * PART, PART), PART)]).start()

        gather.across(s, half).wait_recv()
        keep(s, half, 0).start()
        keep(s, half, 1).start()
        rows = A[pl.ds(pl.multiple_of(u * SHARD, SHARD), SHARD), :]
        out = nn(rows, W[...]).astype(BF16)
        for side in BOTH:
            to = there(s, half, side)
            c, n = cosb[to, :], sinb[to, :]
            mine = out[side * PART : (side + 1) * PART, :]
            for i in range((hq + hk) // HEAD):
                t = mine[:, _head(i)].astype(F32)
                O[to, _head(i)] = (t * c + pltpu.roll(t, HEAD // 2, 1) * n).astype(BF16)
            O[to, hq + hk :] = mine[:, hq + hk :]

    lax.fori_loop(0, QUARTERS * len(BOTH), unit, None)
    puts = [pltpu.make_async_copy(O.at[:, c], t, osem.at[i]) for i, (c, t) in enumerate(zip(cuts, (q_out, k_out, v_out)))]
    for c in puts:
        c.start()
    q, k, v = (O.at[:, c] for c in cuts)

    def rows(iq, _):
        _attend(q, k, v, o, lse, top_s, mix_s, iq, bk)
        gather_y.ring(0, iq).wait_recv()
        gather_y.across(1, iq).start()

    lax.fori_loop(0, len(BOTH), rows, None)
    for c in puts + keep_y:
        c.wait()
    for half in BOTH:
        gather_y.ring(0, half, own[half]).wait_send()
        for s in range(QUARTERS):
            gather.across(s, half).wait_send()
            if s < AWAY[-1]:
                gather.ring(s, half).wait_send()
            if s < len(BOTH):
                gather_y.across(s, half, None if s else own[half]).wait()
            for side in BOTH:
                keep(s, half, side).wait()


def qkv(x, dy, wq, wk, wv, cos, sin, bk=256):
    d, hq, hk, tokens = x.shape[1], wq.shape[1], wk.shape[1], cos.shape[0]
    heads, bq = hq // HEAD, tokens // len(BOTH)
    vmem = pl.BlockSpec(memory_space=pltpu.VMEM)
    return pl.pallas_call(
        functools.partial(_qkv, bk=bk),
        in_specs=[ANY] * 7,
        out_specs=[ANY] * 5 + [vmem] * 2,
        out_shape=[jax.ShapeDtypeStruct((tokens, n), BF16) for n in (hq, hk, hk, d, d, hq)] + [jax.ShapeDtypeStruct((heads, tokens), F32)],
        scratch_shapes=[pltpu.VMEM(x.shape, BF16), pltpu.VMEM(x.shape, BF16), pltpu.VMEM((tokens, d), BF16), pltpu.VMEM((d, hq + 2 * hk), BF16),
                        pltpu.VMEM(cos.shape, F32), pltpu.VMEM(sin.shape, F32), pltpu.VMEM((tokens, hq + 2 * hk), BF16),
                        pltpu.VMEM((heads, bq), F32), pltpu.VMEM((heads, HEAD + 8, bq), F32),
                        *GATHER_SEMS, *GATHER_SEMS, DMA((7,)), DMA((3,)), DMA((5, 2, 2))],
        compiler_params=_params(62, 1),
        cost_estimate=_cost(2 * tokens * d * (hq + 2 * hk), 4 * tokens * d + 2 * d * (hq + 2 * hk)),
        name="gather_qkv",
    )(x, dy, wq, wk, wv, cos, sin)


def _mm_rs(nl, form, arrived, J, tn, lag, after, extra, beside, *refs):
    lhs, rhs, refs = refs[:nl], refs[nl:2 * nl], refs[2 * nl:]
    left, right, refs = (*refs[:2], refs[2:]) if beside else (None, None, refs)
    ins, outs, refs = refs[:extra[0]], refs[extra[0]:sum(extra)], refs[sum(extra):]
    product, refs = (refs[0], refs[1:]) if beside else (None, refs)
    L, refs = refs[:nl], refs[nl:]
    got, refs = refs[:extra[0]], refs[extra[0]:]
    give, refs = refs[:extra[1]], refs[extra[1]:]
    fin, P_, SD, RD, SR, RR, lsem, esem, sd_sem, rd_sem, sr_sem, rr_sem = refs
    g = pl.program_id(0)
    last, slots, waits = J + 3 * lag, 3 * lag + 2, lag + 1
    core, at, partner, nxt, prv = _place()

    def to_partner(j):
        return _send(SD.at[j % 2], RD.at[j % 4], sd_sem.at[j % 2], rd_sem.at[j % 4], partner)

    def to_next(k, j):
        return _send(SR.at[j % waits, k], RR.at[j, k], sr_sem.at[j % waits, k], rr_sem.at[j, k], nxt)

    def half_of(side):
        terms = ((nt if form == "nt" else nn)(l[pl.ds(side * 4 * SHARD, 4 * SHARD), :], r[...]) for l, r in zip(L, rhs))
        return functools.reduce(jnp.add, terms).reshape(4, SHARD, tn)

    def loads(side):
        copies = []
        for i in range(nl):
            for s in range(4):
                for half in BOTH:
                    row = _place_of(s, half, side) if arrived else _owner(at, core, s, side) * SHARD + half * PART
                    copies.append(pltpu.make_async_copy(lhs[i].at[pl.ds(pl.multiple_of(row, PART), PART)],
                                                        L[i].at[pl.ds((side * 4 + s) * SHARD + half * PART, PART)], lsem.at[i, side, s, half]))
        return copies

    extras = [pltpu.make_async_copy(a, b, esem.at[i]) for i, (a, b) in enumerate(zip(ins, got))]

    @pl.when(g == 0)
    def _():
        for side in (1, 0):
            for c in loads(side):
                c.start()
        for c in extras:
            c.start()
        _greet((partner, nxt, prv))
        for c in loads(1):
            c.wait()

    @pl.when(g < J)
    def _():
        SD[g % 2] = half_of(1).astype(BF16)
        to_partner(g).start()

    @pl.when(g == 0)
    def _():
        for c in loads(0):
            c.wait()

    @pl.when((g >= 1) & (g <= J))
    def _():
        j = g - 1
        to_partner(j).wait()
        SR[j % waits, 0] = (P_[j % slots, 1] + RD[j % 4, 1].astype(F32)).astype(BF16)
        to_next(0, j).start()
        for s in (0, 2, 3):
            P_[j % slots, s] += RD[j % 4, s].astype(F32)

    for k, slot in enumerate((2, 3, 0)):
        at_step = 1 + lag * (k + 1)

        @pl.when((g >= at_step) & (g < J + at_step))
        def _():
            j = g - at_step
            to_next(k, j).wait()
            total = P_[j % slots, slot] + RR[j, k].astype(F32)
            if slot:
                SR[j % waits, k + 1] = total.astype(BF16)
                to_next(k + 1, j).start()
            else:
                fin[:, pl.ds(pl.multiple_of(j * tn, tn), tn)] = total

    @pl.when(g < J)
    def _():
        P_[g % slots] = half_of(0)

    if beside:
        later = (last - beside) * 2 // 3

        @pl.when((g >= later) & (g < later + beside))
        def _():
            product[...] = nt(left[...], right[...]).astype(BF16)

    @pl.when(g == last)
    def _():
        for c in extras:
            c.wait()
        after(fin, got, give)
        for i, (a, b) in enumerate(zip(give, outs)):
            pltpu.make_async_copy(a, b, esem.at[i]).start()
        for i, (a, b) in enumerate(zip(give, outs)):
            pltpu.make_async_copy(a, b, esem.at[i]).wait()


def mm_rs(lhs, rhs, form, arrived, after, ins, outs, cid, beside=(), lag=1, tn=512, few=256, vmem=62):
    nl = len(lhs)
    n = rhs[0].shape[1] if form == "nn" else rhs[0].shape[0]
    J = n // tn
    tile = lambda g: jnp.minimum(g, J - 1)
    if form == "nn":
        rspec = [pl.BlockSpec((r.shape[0], tn), lambda g: (0, tile(g))) for r in rhs]
    else:
        rspec = [pl.BlockSpec((tn, r.shape[1]), lambda g: (tile(g), 0)) for r in rhs]
    steps, bspec, pspec, pshape = 0, [], [], []
    if beside:
        left, right = beside
        steps, rows = right.shape[0] // few, left.shape[0] // 2
        part = lambda g: jnp.clip(g - (J + 3 * lag - steps) * 2 // 3, 0, steps - 1)
        bspec = [pl.BlockSpec((rows, left.shape[1]), STILL, pipeline_mode=pl.Buffered(1)), pl.BlockSpec((few, right.shape[1]), lambda g: (part(g), 0))]
        pspec = [pl.BlockSpec((rows, few), lambda g: (0, part(g)))]
        pshape = [jax.ShapeDtypeStruct((rows, right.shape[0]), BF16)]
    return pl.pallas_call(
        functools.partial(_mm_rs, nl, form, arrived, J, tn, lag, after, (len(ins), outs), steps),
        grid=(J + 3 * lag + 1,),
        in_specs=[ANY] * nl + rspec + bspec + [ANY] * len(ins),
        out_specs=[ANY] * outs + pspec,
        out_shape=[jax.ShapeDtypeStruct((SHARD, n), BF16)] * outs + pshape,
        scratch_shapes=[pltpu.VMEM(l.shape, l.dtype) for l in lhs] + [pltpu.VMEM((SHARD, n), BF16)] * (len(ins) + outs) + [
            pltpu.VMEM((SHARD, n), F32),
            pltpu.VMEM((3 * lag + 2, 4, SHARD, tn), F32), pltpu.VMEM((2, 4, SHARD, tn), BF16), pltpu.VMEM((4, 4, SHARD, tn), BF16),
            pltpu.VMEM((lag + 1, 3, SHARD, tn), BF16), pltpu.VMEM((J, 3, SHARD, tn), BF16),
            DMA((nl, 2, 4, 2)), DMA((max(len(ins), outs),)), DMA((2,)), DMA((4,)), DMA((lag + 1, 3)), DMA((J, 3))],
        compiler_params=_params(vmem, cid),
        cost_estimate=_cost(sum(2 * l.size for l in lhs) * n, sum(2 * t.size for t in lhs + rhs)),
        name="mm_rs",
    )(*lhs, *rhs, *beside, *ins)


def _after_wo(total, ins, outs):
    (x,), (h, b) = ins, outs

    def body(i, _):
        r = pl.ds(pl.multiple_of(i * 16, 16), 16)
        new = (x[r, :].astype(F32) + total[r, :].astype(BF16).astype(F32)).astype(BF16)
        h[r, :] = new
        wide = new.astype(F32)
        b[r, :] = (wide * lax.rsqrt(jnp.mean(wide * wide, -1, keepdims=True) + EPS)).astype(BF16)

    lax.fori_loop(0, SHARD // 16, body, None)


def _norm_back(wide, ct):
    scale = lax.rsqrt(jnp.mean(wide * wide, -1, keepdims=True) + EPS)
    along = jnp.mean(ct * wide, -1, keepdims=True)
    return ct * scale - wide * (scale * scale * scale * along)


def _after_norm(total, ins, outs):
    (h, dy), (dh,) = ins, outs

    def body(i, _):
        r = pl.ds(pl.multiple_of(i * 16, 16), 16)
        back = _norm_back(h[r, :].astype(F32), total[r, :].astype(BF16).astype(F32))
        dh[r, :] = (dy[r, :].astype(F32) + back.astype(BF16).astype(F32)).astype(BF16)

    lax.fori_loop(0, SHARD // 16, body, None)


def _finish(x, dh, da, dx):
    back = _norm_back(x[...].astype(F32), da[...].astype(F32))
    dx[...] = (dh[...].astype(F32) + back.astype(BF16).astype(F32)).astype(BF16)


def finish(x, dh, da, rows=16):
    some = _down(rows, x.shape[1])
    return pl.pallas_call(_finish, grid=(x.shape[0] // rows,), in_specs=[some] * 3, out_specs=some, out_shape=jax.ShapeDtypeStruct(x.shape, BF16),
                          compiler_params=_params(56), cost_estimate=_cost(10 * x.size, 8 * x.size), name="finish")(x, dh, da)


def _phase(t, phases):
    at, tile = 0, 0
    for n, first, *_ in phases:
        tile = jnp.where(t >= at, t - at + first, tile)
        at += n
    return tile


def _gate_up(tn, phases, stops, b, dy, wg, wu, hid_out, fu_out, fg_out, b_out, dy_out, B, hid, fu, fg, rs, rr, xs, xr, ys, yr, zs, zr, lsem, bsem, osem):
    t = pl.program_id(0)
    core, at, partner, nxt, prv = _place()
    gather = _Gather(B, (rs, rr, xs, xr), nxt, partner)
    gather_y = _Gather(dy_out, (ys, yr, zs, zr), nxt, partner)
    own = [pl.ds(half * PART, PART) for half in BOTH]
    load = [pltpu.make_async_copy(b.at[own[half]], gather.part(0, half, 0), lsem.at[half]) for half in BOTH]
    keep = lambda s, half: pltpu.make_async_copy(B.at[pl.ds(_place_of(s, half, 0), SHARD)], b_out.at[pl.ds(_place_of(s, half, 0), SHARD)], bsem.at[s, half])

    def whole(s):
        for half in BOTH:
            gather.across(s, half).wait_recv()
            keep(s, half).start()

    @pl.when(t == 0)
    def _():
        for c in load:
            c.start()
        _greet((partner, nxt, prv))
        for half in BOTH:
            load[half].wait()
            gather.ring(0, half).start()
            gather.across(0, half).start()
        whole(0)

    for s in AWAY:
        for half in BOTH:
            @pl.when(t == stops[0][s - 1][half])
            def _():
                gather.ring(s - 1, half).wait_recv()
                if s < AWAY[-1]:
                    gather.ring(s, half).start()
                gather.across(s, half).start()
                if s == AWAY[1] and half:
                    for h in BOTH:
                        gather_y.ring(1, h).start()

            if s > 1:
                @pl.when(t == stops[1][s - 2][half])
                def _():
                    gather_y.ring(s - 1, half).wait_recv()
                    if s < AWAY[-1]:
                        gather_y.ring(s, half).start()
                    gather_y.across(s, half).start()

    slot = t % 2

    def put(u, row, size):
        cols = pl.ds(pl.multiple_of(_phase(u, phases) * tn, tn), tn)
        return [pltpu.make_async_copy(v.at[u % 2, pl.ds(0, size)], o.at[pl.ds(row, size), cols], osem.at[u % 2, i])
                for i, (v, o) in enumerate(((hid, hid_out), (fu, fu_out), (fg, fg_out)))]

    start, ready = 0, 1
    for n, _, row, size in phases:
        @pl.when((t >= start + 2) & (t < start + n + 2))
        def _():
            for c in put(t - 2, row, size):
                c.wait()

        while ready * PAIR < row + size:
            @pl.when(t == start)
            def _():
                whole(ready)

            ready += 1

        @pl.when((t >= start) & (t < start + n))
        def _():
            for m in range(0, size, PAIR):
                rows = B[pl.ds(row + m, PAIR), :]
                gate = nn(rows, wg[...])
                up = nn(rows, wu[...])
                sig = jax.nn.sigmoid(gate)
                act = gate * sig
                to = pl.ds(m, PAIR)
                hid[slot, to, :] = (act * up).astype(BF16)
                fu[slot, to, :] = act
                fg[slot, to, :] = up * (sig * (1 + gate * (1 - sig)))
            for c in put(t, row, size):
                c.start()

        start += n

    @pl.when(t == start - 1)
    def _():
        for u in (start - 2, start - 1):
            for c in put(u, *phases[-1][2:]):
                c.wait()
        for s in range(QUARTERS):
            for half in BOTH:
                gather.across(s, half).wait_send()
                keep(s, half).wait()
                if s > 1:
                    gather_y.across(s, half).wait()
                    gather_y.ring(s - 1, half).wait_send()
                if s < AWAY[-1]:
                    gather.ring(s, half).wait_send()


STOPS = (((4, 8), (11, 13), (16, 18)), ((21, 23), (25, 27)))


def gate_up(b, dy, wg, wu, tn=256, early=9, second=4):
    (shard, d), n = b.shape, wg.shape[1]
    tokens, J = 8 * shard, n // tn
    quarter, half = tokens // 4, tokens // 2
    phases = ((early, 0, 0, quarter), (J - early, early, 0, half), (second, 0, quarter, half), (second, 0, tokens - quarter, quarter),
              (early - second, second, quarter, tokens - quarter), (J - early, early, half, half))
    tile = pl.BlockSpec((d, tn), lambda t: (0, _phase(t, phases)))
    stage = [pltpu.VMEM((2, tokens - quarter, tn), w) for w in (BF16, F32, F32)]
    return pl.pallas_call(
        functools.partial(_gate_up, tn, phases, STOPS),
        grid=(sum(p[0] for p in phases),),
        in_specs=[ANY, ANY, tile, tile],
        out_specs=[ANY] * 5,
        out_shape=[jax.ShapeDtypeStruct((tokens, m), w) for m, w in ((n, BF16), (n, F32), (n, F32), (d, BF16), (d, BF16))],
        scratch_shapes=[pltpu.VMEM((tokens, d), BF16), *stage, *GATHER_SEMS, *GATHER_SEMS, DMA((2,)), DMA((4, 2)), DMA((2, 3))],
        input_output_aliases={1: 4},
        compiler_params=_params(62, 3),
        cost_estimate=_cost(4 * tokens * d * n, 12 * d * n + 10 * tokens * n + 8 * tokens * d, tokens * n),
        name="gather_gate_up",
    )(b, dy, wg, wu)


def _d_hidden(dy, wd, early, fu, fg, dg, du):
    half = dy.shape[0]
    late = nt(dy[...], wd[...]).astype(BF16)
    for rows, d in ((slice(0, half), early[...]), (slice(half, 2 * half), late)):
        d = d.astype(F32)
        dg[rows, :] = (d * fg[rows, :]).astype(BF16)
        du[rows, :] = (d * fu[rows, :]).astype(BF16)


def d_hidden(dy, wd, early, fu, fg, tn=256):
    tokens, d = dy.shape
    n, half = wd.shape[0], tokens // 2
    cols = _along(tokens, tn)
    return pl.pallas_call(
        _d_hidden,
        grid=(n // tn,),
        in_specs=[pl.BlockSpec((half, d), lambda i: (1, 0), pipeline_mode=pl.Buffered(1)), _down(tn, d), _along(half, tn), cols, cols],
        out_specs=[cols, cols],
        out_shape=[jax.ShapeDtypeStruct((tokens, n), BF16)] * 2,
        compiler_params=_params(60),
        cost_estimate=_cost(tokens * d * n, d * (tokens + 2 * n) + 13 * tokens * n),
        name="d_hidden",
    )(dy, wd, early, fu, fg)


def _da(dq, dkv, wq, wk, wv, out, kv):
    kv[:, :HEAD] = wk[...]
    kv[:, HEAD:] = wv[...]
    out[...] = (nt(dq[...], wq[...]) + nt(dkv[...], kv[...])).astype(BF16)


def d_states(dq, dkv, wq, wk, wv, tn=1024):
    tokens, hq = dq.shape
    d = wq.shape[0]
    whole = lambda t: pl.BlockSpec(t.shape, STILL)
    some = lambda t: _down(tn, t.shape[1])
    return pl.pallas_call(
        _da,
        grid=(d // tn,),
        in_specs=[whole(dq), whole(dkv), some(wq), some(wk), some(wv)],
        out_specs=_along(tokens, tn),
        out_shape=jax.ShapeDtypeStruct((tokens, d), BF16),
        scratch_shapes=[pltpu.VMEM((tn, 2 * HEAD), BF16)],
        compiler_params=_params(56),
        cost_estimate=_cost(2 * tokens * d * (hq + 2 * HEAD), 2 * d * (tokens + hq + 2 * HEAD)),
        name="d_states",
    )(dq, dkv, wq, wk, wv)


def _outer(tasks, *refs):
    i = pl.program_id(0)
    for first, last, a, ts, outs in tasks:
        @pl.when((i >= first) & (i < last))
        def _():
            for t, own in zip(ts, outs):
                whole = tt(refs[a][...], refs[t][...]).astype(BF16)
                at = 0
                for n in own:
                    refs[n][...] = whole[:, at : at + refs[n].shape[1]]
                    at += refs[n].shape[1]


def outer(*tasks, vmem=62):
    ins, in_specs, out_shape, out_specs, plan, results = [], [], [], [], [], []
    step = 0
    for a, ts, tm, tn, *cuts in tasks:
        cuts = cuts or [(t.shape[1],) for t in ts]
        m, n = a.shape[1] // tm, ts[0].shape[1] // tn if tn else 1

        def at(i, step=step, m=m, n=n):
            k = jnp.clip(i - step, 0, m * n - 1)
            return k % m, k // m

        row = lambda i, at=at: (0, at(i)[0])
        column = lambda i, at=at: (0, at(i)[1])
        plan.append([step, step + m * n, len(ins), range(len(ins) + 1, len(ins) + 1 + len(ts)), []])
        ins += [a, *ts]
        in_specs += [pl.BlockSpec((a.shape[0], tm), row)] + [pl.BlockSpec((a.shape[0], tn or t.shape[1]), column) for t in ts]
        for t, widths in zip(ts, cuts):
            plan[-1][-1].append(range(len(out_shape), len(out_shape) + len(widths)))
            out_shape += [jax.ShapeDtypeStruct((a.shape[1], w), BF16) for w in widths]
            out_specs += [pl.BlockSpec((tm, tn or w), at) for w in widths]
        step += m * n
    plan = [(f, l, a, ts, [[len(ins) + n for n in own] for own in outs]) for f, l, a, ts, outs in plan]
    return pl.pallas_call(
        functools.partial(_outer, plan),
        grid=(step,),
        in_specs=in_specs,
        out_specs=out_specs,
        out_shape=out_shape,
        compiler_params=_params(vmem),
        cost_estimate=_cost(sum(2 * a.size * t.shape[1] for a, ts, *_ in tasks for t in ts), sum(2 * t.size for t in ins + out_shape)),
        name="outer",
    )(*ins)


def tables(tokens):
    half = HEAD // 2
    angle = np.arange(tokens, dtype=np.float32)[:, None] * np.float32(THETA) ** (-np.arange(half, dtype=np.float32) / np.float32(half))
    cos, sin = np.cos(angle), np.sin(angle)
    return jnp.asarray(np.concatenate([cos, cos], -1)), jnp.asarray(np.concatenate([-sin, sin], -1))


def layer_grads(x, dy, wq, wk, wv, wo, wg, wu, wd):
    cos, sin = tables(8 * x.shape[0])
    q, k, v, a, dy_all, o, lse = qkv(x, dy, wq, wk, wv, cos, sin)
    h, b, early = mm_rs([o], [wo], "nn", False, _after_wo, [x], 2, 2, beside=(dy_all, wd), lag=2)
    hidden, fu, fg, b, dy_all = gate_up(b, dy_all, wg, wu)
    dgate, dup = d_hidden(dy_all, wd, early, fu, fg)
    (dh,) = mm_rs([dgate, dup], [wg, wu], "nt", True, _after_norm, [h, dy], 1, 4)
    dh_all = lax.all_gather(dh, "tp", axis=0, tiled=True)
    by_gate, by_up = outer((b, [dgate, dup], 1024, 1792))
    dh_all, by_gate, by_up = lax.optimization_barrier((dh_all, by_gate, by_up))
    d_o = nt(dh_all, wo).astype(BF16)
    dq, dkv = attend_bwd(q, k, v, d_o, o, lse, cos, sin)
    da = lax.psum_scatter(d_states(dq, dkv, wq, wk, wv), "tp", scatter_dimension=0, tiled=True)
    by_down, by_o, by_q, by_k, by_v = outer(
        (hidden, [dy_all], 1792, 1024), (o, [dh_all], 1024, 1024), (a, [dq, dkv], 1024, None, (dq.shape[1],), (HEAD, HEAD)))
    return finish(x, dh, da), by_q, by_k, by_v, by_o, by_gate, by_up, by_down


def solution(mesh):
    def step(x, dy, *weights):
        by_x, *by_w = layer_grads(x[0], dy[0], *weights)
        return (by_x[None], *by_w)

    states, by_columns, by_rows = P("dp", "tp", None), P(None, "tp"), P("tp", None)
    weights = (by_columns, by_columns, by_columns, by_rows, by_columns, by_columns, by_rows)
    own = tuple(P("dp", "tp") if spec == by_columns else P(("dp", "tp"), None) for spec in weights)
    return jax.shard_map(step, mesh=mesh, in_specs=(states, states, *weights), out_specs=(states, *own), check_vma=False)
```

```python
import functools

import jax
import jax.numpy as jnp
import numpy as np
from jax import lax
from jax.experimental import pallas as pl
from jax.experimental.pallas import tpu as pltpu
from jax.sharding import PartitionSpec as P

HEAD = 128
THETA = 10000
SHARD = 128
PART = SHARD // 2
PAIR = 2 * SHARD
MESH = pl.DeviceIdType.MESH
DMA = pltpu.SemaphoreType.DMA
F32, BF16 = jnp.float32, jnp.bfloat16
ANY = pl.BlockSpec(memory_space=pl.ANY)
EPS = 1e-6
MIB = 2**20
BOTH, AWAY, QUARTERS = range(2), range(1, 4), 4
STILL = lambda *_: (0, 0)
NEG = -1e30
HIDDEN = 2 * NEG
LOG2E = 1.4426950408889634


def _contract(ca, cb):
    return lambda a, b: lax.dot_general(a, b, (((ca,), (cb,)), ((), ())), preferred_element_type=F32)


nn, nt, tt = _contract(1, 0), _contract(1, 1), _contract(0, 0)


def _slot(i):
    return i % 2


def _pair(*shape, dtype=BF16):
    return pltpu.VMEM((2, *shape), dtype)


def _params(vmem, cid=None, **more):
    if cid is not None:
        more |= {"collective_id": cid, "has_side_effects": True}
    return pltpu.CompilerParams(vmem_limit_bytes=vmem * MIB, **more)


def _down(rows, columns):
    return pl.BlockSpec((rows, columns), lambda i: (i, 0))


def _along(rows, columns):
    return pl.BlockSpec((rows, columns), lambda i: (0, i))


def _cost(products, *arrays):
    return pl.CostEstimate(flops=products + products, transcendentals=0, bytes_accessed=sum(t.size * t.dtype.itemsize for t in arrays))


def _hidden(first_key, first_query, bk, bq):
    keys = lax.broadcasted_iota(jnp.int32, (bk, bq), 0) + first_key
    return keys > lax.broadcasted_iota(jnp.int32, (bk, bq), 1) + first_query


def _head(n):
    return slice(n * HEAD, (n + 1) * HEAD)


def _blocks(block, iq, n):
    lax.fori_loop(0, iq * n, lambda j, _: block(j, False), None)
    lax.fori_loop(iq * n, (iq + 1) * n, lambda j, _: block(j, True), None)


def _attend(q, k, v, o, lse, top_s, mix_s, iq, bk):
    bq, heads = top_s.shape[1], top_s.shape[0]
    scale = HEAD**-0.5
    e = scale * LOG2E
    rows = pl.ds(pl.multiple_of(iq * bq, bq), bq)
    top_s[...] = jnp.full(top_s.shape, NEG, F32)
    mix_s[...] = jnp.zeros(mix_s.shape, F32)
    ones = jnp.ones((mix_s.shape[1] - HEAD, bk), BF16)

    def block(j, masked):
        here = pl.ds(pl.multiple_of(j * bk, bk), bk)
        scores = [nt(k[here, :], q[rows, _head(n)]) for n in range(heads)]
        hide = _hidden(j * bk, iq * bq, bk, bq) if masked else None
        weights, keeps = [], []
        for n, s in enumerate(scores):
            if masked:
                s = jnp.where(hide, HIDDEN, s)
            old = top_s[n : n + 1, :]
            top = jnp.maximum(old, s.max(axis=0, keepdims=True))
            top_s[n : n + 1, :] = top
            weights.append(jnp.exp2((s - top) * e).astype(BF16))
            keeps.append(jnp.exp2((old - top) * e))
        values = jnp.concatenate([v[here, :].T, ones], axis=0)
        for n in range(heads):
            mix_s[n] = mix_s[n] * keeps[n] + nn(values, weights[n])

    _blocks(block, iq, bq // bk)
    for n in range(heads):
        total = mix_s[n, HEAD : HEAD + 1, :]
        o[rows, _head(n)] = (mix_s[n, :HEAD, :] * (1 / total)).T.astype(BF16)
        lse[n : n + 1, rows] = top_s[n : n + 1, :] * scale + jnp.log(total)


def _unturned(t, c, n):
    t = t.astype(BF16).astype(F32)
    return (t * c - pltpu.roll(t, HEAD // 2, 1) * n).astype(BF16)


def _attend_bwd(q_ref, k_ref, v_ref, do_ref, o_ref, lse_ref, cos_ref, sin_ref, cosk_ref, sink_ref, dq_ref, dkv_ref, dq_s, dk_s, dv_s, delta_s, *, bk):
    bq, heads = q_ref.shape[0], q_ref.shape[1] // HEAD
    iq = pl.program_id(0)
    scale = HEAD**-0.5
    e = scale * LOG2E

    @pl.when(iq == 0)
    def _():
        dk_s[...] = jnp.zeros_like(dk_s)
        dv_s[...] = jnp.zeros_like(dv_s)

    dq_s[...] = jnp.zeros_like(dq_s)
    for n in range(heads):
        both = do_ref[:, _head(n)].astype(F32) * o_ref[:, _head(n)].astype(F32)
        delta_s[n : n + 1, :] = both.T.sum(axis=0, keepdims=True)

    def block(j, masked):
        here = pl.ds(pl.multiple_of(j * bk, bk), bk)
        scores = [nt(k_ref[here, :], q_ref[:, _head(n)]) for n in range(heads)]
        dps = [nt(v_ref[here, :], do_ref[:, _head(n)]) for n in range(heads)]
        hide = _hidden(j * bk, iq * bq, bk, bq) if masked else None
        for n in range(heads):
            p = jnp.exp2(scores[n] * e - lse_ref[n : n + 1, :] * LOG2E)
            if masked:
                p = jnp.where(hide, 0.0, p)
            ds = (p * (dps[n] - delta_s[n : n + 1, :])).astype(BF16)
            dv_s[here, :] += nn(p.astype(BF16), do_ref[:, _head(n)])
            dk_s[here, :] += nn(ds, q_ref[:, _head(n)])
            dq_s[n] += nn(k_ref[here, :].T, ds)

    _blocks(block, iq, bq // bk)
    for n in range(heads):
        dq_ref[:, _head(n)] = _unturned((dq_s[n] * scale).T, cos_ref[...], sin_ref[...])

    @pl.when(iq == pl.num_programs(0) - 1)
    def _():
        dkv_ref[:, :HEAD] = _unturned(dk_s[...] * scale, cosk_ref[...], sink_ref[...])
        dkv_ref[:, HEAD:] = dv_s[...].astype(BF16)


def attend_bwd(q, k, v, d_o, o, lse, cos, sin, bq=256, bk=256):
    tokens, d = q.shape
    heads = d // HEAD
    rows = _down(bq, d)
    some, every = _down(bq, HEAD), pl.BlockSpec((tokens, HEAD), STILL)
    return pl.pallas_call(
        functools.partial(_attend_bwd, bk=bk),
        grid=(tokens // bq,),
        in_specs=[rows, every, every, rows, rows, _along(heads, bq), some, some, every, every],
        out_specs=[rows, pl.BlockSpec((tokens, 2 * HEAD), STILL)],
        out_shape=[jax.ShapeDtypeStruct((tokens, d), BF16), jax.ShapeDtypeStruct((tokens, 2 * HEAD), BF16)],
        scratch_shapes=[pltpu.VMEM((heads, HEAD, bq), F32), pltpu.VMEM((tokens, HEAD), F32), pltpu.VMEM((tokens, HEAD), F32), pltpu.VMEM((heads, bq), F32)],
        compiler_params=_params(56),
        cost_estimate=_cost(5 * tokens * tokens * d, q, d_o, o, q),
        name="attend_bwd",
    )(q, k, v, d_o, o, lse, cos, sin, cos, sin)


def _flip(c):
    return c + (c // 2) * (1 - 2 * (_slot(c)))


def _place():
    me = lax.axis_index("tp")
    core, pos = me % 2, _flip(me // 2)
    turn = 1 - 2 * core
    at = lambda k, c: _flip((pos + turn * k + 8) % 4) * 2 + c
    return core, at, me + turn, at(1, core), at(-1, core)


def _owner(at, core, s, side):
    return at(-s if side == 0 else s, core if side == 0 else 1 - core)


def _greet(devices):
    barrier = pltpu.get_barrier_semaphore()
    for d in devices:
        pl.semaphore_signal(barrier, inc=1, device_id={"tp": d}, device_id_type=MESH)
    pl.semaphore_wait(barrier, len(devices))


def _send(src, dst, ssem, rsem, dev):
    return pltpu.make_async_remote_copy(src_ref=src, dst_ref=dst, send_sem=ssem, recv_sem=rsem, device_id={"tp": dev}, device_id_type=MESH)


def _place_of(s, half, side):
    return ((s * 2 + half) * 2 + side) * PART


class _Gather:
    def __init__(self, ref, sems, nxt, partner):
        self.ref, self.sems, self.nxt, self.partner = ref, sems, nxt, partner

    def part(self, s, half, side):
        return self.ref.at[pl.ds(pl.multiple_of(_place_of(s, half, side), PART), PART)]

    def ring(self, s, half, src=None):
        rs, rr, _, _ = self.sems
        return _send(self.part(s, half, 0) if src is None else src, self.part(s + 1, half, 0), rs.at[s, half], rr.at[s + 1, half], self.nxt)

    def across(self, s, half, src=None):
        _, _, xs, xr = self.sems
        return _send(self.part(s, half, 0) if src is None else src, self.part(s, half, 1), xs.at[s, half], xr.at[s, half], self.partner)


GATHER_SEMS = [DMA((4, 2))] * 4


def _norm_rows(src, dst, at_row, rows, step=16):
    def body(i, _):
        r = pl.multiple_of(i * step, step)
        wide = src[pl.ds(r, step), :].astype(F32)
        scale = lax.rsqrt(jnp.mean(wide * wide, -1, keepdims=True) + EPS)
        dst[pl.ds(pl.multiple_of(at_row(r), step), step), :] = (wide * scale).astype(BF16)

    lax.fori_loop(rows[0] // step, rows[1] // step, body, None)


def _qkv(x, dy, wq, wk, wv, cos, sin, q_out, k_out, v_out, a_out, y_out, o, lse, xb, yb, A, W, cosb, sinb, O, top_s, mix_s,
         rs, rr, xs, xr, ys, yr, zs, zr, lsem, osem, asem, bk):
    core, at, partner, nxt, prv = _place()
    gather = _Gather(A, (rs, rr, xs, xr), nxt, partner)
    gather_y = _Gather(y_out, (ys, yr, zs, zr), nxt, partner)
    hq = wq.shape[1]
    hk = wk.shape[1]
    cuts = (pl.ds(0, hq), pl.ds(hq, hk), pl.ds(hq + hk, hk))
    moves = ((x, xb), (cos, cosb), (sin, sinb), *((w, W.at[:, c]) for w, c in zip((wq, wk, wv), cuts)), (dy, yb))
    loads = [pltpu.make_async_copy(a, b, lsem.at[i]) for i, (a, b) in enumerate(moves)]
    for c in loads:
        c.start()
    _greet((partner, nxt, prv))
    loads[0].wait()
    own = [yb.at[pl.ds(half * PART, PART)] for half in BOTH]
    keep_y = [pltpu.make_async_copy(own[half], gather_y.part(0, half, 0), asem.at[QUARTERS, half, 0]) for half in BOTH]
    for half in BOTH:
        _norm_rows(xb, A, lambda r: r + half * PART, (half * PART, half * PART + PART))
        gather.ring(0, half).start()
        gather.across(0, half).start()
    for c in loads[1:]:
        c.wait()
    for half in BOTH:
        keep_y[half].start()
        gather_y.across(0, half, own[half]).start()

    def there(s, half, side):
        return pl.ds(pl.multiple_of(_owner(at, core, s, side) * SHARD + half * PART, PART), PART)

    def keep(s, half, side):
        return pltpu.make_async_copy(gather.part(s, half, side), a_out.at[there(s, half, side)], asem.at[s, half, side])

    def unit(u, _):
        s, half = u // 2, u % 2

        @pl.when(s > 0)
        def _():
            gather.ring(s - 1, half).wait_recv()

            @pl.when(s < AWAY[-1])
            def _():
                gather.ring(s, half).start()

            gather.across(s, half).start()

        @pl.when(s == AWAY[-1])
        def _():
            gather_y.ring(0, half, yb.at[pl.ds(pl.multiple_of(half * PART, PART), PART)]).start()

        gather.across(s, half).wait_recv()
        keep(s, half, 0).start()
        keep(s, half, 1).start()
        rows = A[pl.ds(pl.multiple_of(u * SHARD, SHARD), SHARD), :]
        out = nn(rows, W[...]).astype(BF16)
        for side in BOTH:
            to = there(s, half, side)
            c, n = cosb[to, :], sinb[to, :]
            mine = out[side * PART : (side + 1) * PART, :]
            for i in range((hq + hk) // HEAD):
                t = mine[:, _head(i)].astype(F32)
                O[to, _head(i)] = (t * c + pltpu.roll(t, HEAD // 2, 1) * n).astype(BF16)
            O[to, hq + hk :] = mine[:, hq + hk :]

    lax.fori_loop(0, QUARTERS * len(BOTH), unit, None)
    puts = [pltpu.make_async_copy(O.at[:, c], t, osem.at[i]) for i, (c, t) in enumerate(zip(cuts, (q_out, k_out, v_out)))]
    for c in puts:
        c.start()
    q, k, v = (O.at[:, c] for c in cuts)

    def rows(iq, _):
        _attend(q, k, v, o, lse, top_s, mix_s, iq, bk)
        gather_y.ring(0, iq).wait_recv()
        gather_y.across(1, iq).start()

    lax.fori_loop(0, len(BOTH), rows, None)
    for c in puts + keep_y:
        c.wait()
    for half in BOTH:
        gather_y.ring(0, half, own[half]).wait_send()
        for s in range(QUARTERS):
            gather.across(s, half).wait_send()
            if s < AWAY[-1]:
                gather.ring(s, half).wait_send()
            if s < len(BOTH):
                gather_y.across(s, half, None if s else own[half]).wait()
            for side in BOTH:
                keep(s, half, side).wait()


def qkv(x, dy, wq, wk, wv, cos, sin, bk=256):
    d, hq, hk, tokens = x.shape[1], wq.shape[1], wk.shape[1], cos.shape[0]
    heads, bq = hq // HEAD, tokens // len(BOTH)
    vmem = pl.BlockSpec(memory_space=pltpu.VMEM)
    return pl.pallas_call(
        functools.partial(_qkv, bk=bk),
        in_specs=[ANY] * 7,
        out_specs=[ANY] * 5 + [vmem] * 2,
        out_shape=[jax.ShapeDtypeStruct((tokens, n), BF16) for n in (hq, hk, hk, d, d, hq)] + [jax.ShapeDtypeStruct((heads, tokens), F32)],
        scratch_shapes=[pltpu.VMEM(x.shape, BF16), pltpu.VMEM(x.shape, BF16), pltpu.VMEM((tokens, d), BF16), pltpu.VMEM((d, hq + 2 * hk), BF16),
                        pltpu.VMEM(cos.shape, F32), pltpu.VMEM(sin.shape, F32), pltpu.VMEM((tokens, hq + 2 * hk), BF16),
                        pltpu.VMEM((heads, bq), F32), pltpu.VMEM((heads, HEAD + 8, bq), F32),
                        *GATHER_SEMS, *GATHER_SEMS, DMA((7,)), DMA((3,)), DMA((5, 2, 2))],
        compiler_params=_params(62, 1),
        cost_estimate=_cost(tokens * d * hq, x, dy, wq, wk, wv),
        name="gather_qkv",
    )(x, dy, wq, wk, wv, cos, sin)


def _mm_rs(nl, form, arrived, J, tn, lag, after, extra, beside, *refs):
    lhs, rhs, refs = refs[:nl], refs[nl:2 * nl], refs[2 * nl:]
    left, right, refs = (*refs[:2], refs[2:]) if beside else (None, None, refs)
    ins, outs, refs = refs[:extra[0]], refs[extra[0]:sum(extra)], refs[sum(extra):]
    product, refs = (refs[0], refs[1:]) if beside else (None, refs)
    L, refs = refs[:nl], refs[nl:]
    got, refs = refs[:extra[0]], refs[extra[0]:]
    give, refs = refs[:extra[1]], refs[extra[1]:]
    fin, P_, SD, RD, SR, RR, lsem, esem, sd_sem, rd_sem, sr_sem, rr_sem = refs
    g = pl.program_id(0)
    last, slots, waits = J + 3 * lag, 3 * lag + 2, lag + 1
    core, at, partner, nxt, prv = _place()

    def to_partner(j):
        return _send(SD.at[_slot(j)], RD.at[j % 4], sd_sem.at[_slot(j)], rd_sem.at[j % 4], partner)

    def to_next(k, j):
        return _send(SR.at[j % waits, k], RR.at[j, k], sr_sem.at[j % waits, k], rr_sem.at[j, k], nxt)

    def half_of(side):
        terms = ((nt if form == "nt" else nn)(l[pl.ds(side * 4 * SHARD, 4 * SHARD), :], r[...]) for l, r in zip(L, rhs))
        return functools.reduce(jnp.add, terms).reshape(4, SHARD, tn)

    def loads(side):
        copies = []
        for i in range(nl):
            for s in range(4):
                for half in BOTH:
                    row = _place_of(s, half, side) if arrived else _owner(at, core, s, side) * SHARD + half * PART
                    copies.append(pltpu.make_async_copy(lhs[i].at[pl.ds(pl.multiple_of(row, PART), PART)],
                                                        L[i].at[pl.ds((side * 4 + s) * SHARD + half * PART, PART)], lsem.at[i, side, s, half]))
        return copies

    extras = [pltpu.make_async_copy(a, b, esem.at[i]) for i, (a, b) in enumerate(zip(ins, got))]

    @pl.when(g == 0)
    def _():
        for side in (1, 0):
            for c in loads(side):
                c.start()
        for c in extras:
            c.start()
        _greet((partner, nxt, prv))
        for c in loads(1):
            c.wait()

    @pl.when(g < J)
    def _():
        SD[_slot(g)] = half_of(1).astype(BF16)
        to_partner(g).start()

    @pl.when(g == 0)
    def _():
        for c in loads(0):
            c.wait()

    @pl.when((g >= 1) & (g <= J))
    def _():
        j = g - 1
        to_partner(j).wait()
        SR[j % waits, 0] = (P_[j % slots, 1] + RD[j % 4, 1].astype(F32)).astype(BF16)
        to_next(0, j).start()
        for s in (0, 2, 3):
            P_[j % slots, s] += RD[j % 4, s].astype(F32)

    for k, slot in enumerate((2, 3, 0)):
        at_step = 1 + lag * (k + 1)

        @pl.when((g >= at_step) & (g < J + at_step))
        def _():
            j = g - at_step
            to_next(k, j).wait()
            total = P_[j % slots, slot] + RR[j, k].astype(F32)
            if slot:
                SR[j % waits, k + 1] = total.astype(BF16)
                to_next(k + 1, j).start()
            else:
                fin[:, pl.ds(pl.multiple_of(j * tn, tn), tn)] = total

    @pl.when(g < J)
    def _():
        P_[g % slots] = half_of(0)

    if beside:
        later = (last - beside) * 2 // 3

        @pl.when((g >= later) & (g < later + beside))
        def _():
            product[...] = nt(left[...], right[...]).astype(BF16)

    @pl.when(g == last)
    def _():
        for c in extras:
            c.wait()
        after(fin, got, give)
        for i, (a, b) in enumerate(zip(give, outs)):
            pltpu.make_async_copy(a, b, esem.at[i]).start()
        for i, (a, b) in enumerate(zip(give, outs)):
            pltpu.make_async_copy(a, b, esem.at[i]).wait()


def mm_rs(lhs, rhs, form, arrived, after, ins, outs, cid, beside=(), lag=1, tn=512, few=256, vmem=62):
    nl = len(lhs)
    n = rhs[0].shape[1] if form == "nn" else rhs[0].shape[0]
    J = n // tn
    tile = lambda g: jnp.minimum(g, J - 1)
    if form == "nn":
        rspec = [pl.BlockSpec((r.shape[0], tn), lambda g: (0, tile(g))) for r in rhs]
    else:
        rspec = [pl.BlockSpec((tn, r.shape[1]), lambda g: (tile(g), 0)) for r in rhs]
    steps, bspec, pspec, pshape = 0, [], [], []
    if beside:
        left, right = beside
        steps, rows = right.shape[0] // few, left.shape[0] // 2
        part = lambda g: jnp.clip(g - (J + 3 * lag - steps) * 2 // 3, 0, steps - 1)
        bspec = [pl.BlockSpec((rows, left.shape[1]), STILL, pipeline_mode=pl.Buffered(1)), pl.BlockSpec((few, right.shape[1]), lambda g: (part(g), 0))]
        pspec = [pl.BlockSpec((rows, few), lambda g: (0, part(g)))]
        pshape = [jax.ShapeDtypeStruct((rows, right.shape[0]), BF16)]
    return pl.pallas_call(
        functools.partial(_mm_rs, nl, form, arrived, J, tn, lag, after, (len(ins), outs), steps),
        grid=(J + 3 * lag + 1,),
        in_specs=[ANY] * nl + rspec + bspec + [ANY] * len(ins),
        out_specs=[ANY] * outs + pspec,
        out_shape=[jax.ShapeDtypeStruct((SHARD, n), BF16)] * outs + pshape,
        scratch_shapes=[pltpu.VMEM(l.shape, l.dtype) for l in lhs] + [pltpu.VMEM((SHARD, n), BF16)] * (len(ins) + outs) + [
            pltpu.VMEM((SHARD, n), F32),
            pltpu.VMEM((3 * lag + 2, 4, SHARD, tn), F32), _pair(4, SHARD, tn), pltpu.VMEM((4, 4, SHARD, tn), BF16),
            pltpu.VMEM((lag + 1, 3, SHARD, tn), BF16), pltpu.VMEM((J, 3, SHARD, tn), BF16),
            DMA((nl, 2, 4, 2)), DMA((max(len(ins), outs),)), DMA((2,)), DMA((4,)), DMA((lag + 1, 3)), DMA((J, 3))],
        compiler_params=_params(vmem, cid),
        cost_estimate=_cost(sum(l.size for l in lhs) * n, *lhs, *rhs),
        name="mm_rs",
    )(*lhs, *rhs, *beside, *ins)


def _after_wo(total, ins, outs):
    (x,), (h, b) = ins, outs

    def body(i, _):
        r = pl.ds(pl.multiple_of(i * 16, 16), 16)
        new = (x[r, :].astype(F32) + total[r, :].astype(BF16).astype(F32)).astype(BF16)
        h[r, :] = new
        wide = new.astype(F32)
        b[r, :] = (wide * lax.rsqrt(jnp.mean(wide * wide, -1, keepdims=True) + EPS)).astype(BF16)

    lax.fori_loop(0, SHARD // 16, body, None)


def _norm_back(wide, ct):
    scale = lax.rsqrt(jnp.mean(wide * wide, -1, keepdims=True) + EPS)
    along = jnp.mean(ct * wide, -1, keepdims=True)
    return ct * scale - wide * (scale * scale * scale * along)


def _after_norm(total, ins, outs):
    (h, dy), (dh,) = ins, outs

    def body(i, _):
        r = pl.ds(pl.multiple_of(i * 16, 16), 16)
        back = _norm_back(h[r, :].astype(F32), total[r, :].astype(BF16).astype(F32))
        dh[r, :] = (dy[r, :].astype(F32) + back.astype(BF16).astype(F32)).astype(BF16)

    lax.fori_loop(0, SHARD // 16, body, None)


def _finish(x, dh, da, dx):
    back = _norm_back(x[...].astype(F32), da[...].astype(F32))
    dx[...] = (dh[...].astype(F32) + back.astype(BF16).astype(F32)).astype(BF16)


def finish(x, dh, da, rows=16):
    some = _down(rows, x.shape[1])
    return pl.pallas_call(_finish, grid=(x.shape[0] // rows,), in_specs=[some] * 3, out_specs=some, out_shape=jax.ShapeDtypeStruct(x.shape, BF16),
                          compiler_params=_params(56), cost_estimate=_cost(x.size, x, x, x, x), name="finish")(x, dh, da)


def _phase(t, phases):
    at, tile = 0, 0
    for n, first, *_ in phases:
        tile = jnp.where(t >= at, t - at + first, tile)
        at += n
    return tile


def _gate_up(tn, phases, stops, b, dy, wg, wu, early, hid_out, dg_out, du_out, fu_out, fg_out, b_out, dy_out, B, hid, dg, du, fu, fg, rs, rr, xs, xr, ys, yr, zs, zr, lsem, bsem, osem):
    t = pl.program_id(0)
    core, at, partner, nxt, prv = _place()
    gather = _Gather(B, (rs, rr, xs, xr), nxt, partner)
    gather_y = _Gather(dy_out, (ys, yr, zs, zr), nxt, partner)
    own = [pl.ds(half * PART, PART) for half in BOTH]
    load = [pltpu.make_async_copy(b.at[own[half]], gather.part(0, half, 0), lsem.at[half]) for half in BOTH]
    keep = lambda s, half: pltpu.make_async_copy(B.at[pl.ds(_place_of(s, half, 0), SHARD)], b_out.at[pl.ds(_place_of(s, half, 0), SHARD)], bsem.at[s, half])

    def whole(s):
        for half in BOTH:
            gather.across(s, half).wait_recv()
            keep(s, half).start()

    @pl.when(t == 0)
    def _():
        for c in load:
            c.start()
        _greet((partner, nxt, prv))
        for half in BOTH:
            load[half].wait()
            gather.ring(0, half).start()
            gather.across(0, half).start()
        whole(0)

    for s in AWAY:
        for half in BOTH:
            @pl.when(t == stops[0][s - 1][half])
            def _():
                gather.ring(s - 1, half).wait_recv()
                if s < AWAY[-1]:
                    gather.ring(s, half).start()
                gather.across(s, half).start()
                if s == AWAY[1] and half:
                    for h in BOTH:
                        gather_y.ring(1, h).start()

            if s > 1:
                @pl.when(t == stops[1][s - 2][half])
                def _():
                    gather_y.ring(s - 1, half).wait_recv()
                    if s < AWAY[-1]:
                        gather_y.ring(s, half).start()
                    gather_y.across(s, half).start()

    slot = t % 2

    half = fu_out.shape[0]

    def put(u, row, size):
        cols = pl.ds(pl.multiple_of(_phase(u, phases) * tn, tn), tn)
        copies = []
        for c, m in enumerate(range(0, size, PAIR)):
            r = row + m
            late = r >= half
            to = ((hid, hid_out, r), (fu, fu_out, r - half), (fg, fg_out, r - half)) if late else ((hid, hid_out, r), (du, du_out, r), (dg, dg_out, r))
            copies += [pltpu.make_async_copy(v.at[_slot(u), pl.ds(m, PAIR)], o.at[pl.ds(at, PAIR), cols], osem.at[_slot(u), c, i]) for i, (v, o, at) in enumerate(to)]
        return copies

    start, ready = 0, 1
    for n, _, row, size in phases:
        @pl.when((t >= start + 2) & (t < start + n + 2))
        def _():
            for c in put(t - 2, row, size):
                c.wait()

        while ready * PAIR < row + size:
            @pl.when(t == start)
            def _():
                whole(ready)

            ready += 1

        @pl.when((t >= start) & (t < start + n))
        def _():
            for m in range(0, size, PAIR):
                rows = B[pl.ds(row + m, PAIR), :]
                gate = nn(rows, wg[...])
                up = nn(rows, wu[...])
                sig = jax.nn.sigmoid(gate)
                act = gate * sig
                to = pl.ds(m, PAIR)
                hid[slot, to, :] = (act * up).astype(BF16)
                slope = up * (sig * (1 + gate * (1 - sig)))
                if row + m < half:
                    d = early[pl.ds(row + m, PAIR), :].astype(F32)
                    du[slot, to, :] = (d * act).astype(BF16)
                    dg[slot, to, :] = (d * slope).astype(BF16)
                else:
                    fu[slot, to, :] = act
                    fg[slot, to, :] = slope
            for c in put(t, row, size):
                c.start()

        start += n

    @pl.when(t == start - 1)
    def _():
        for u in (start - 2, start - 1):
            for c in put(u, *phases[-1][2:]):
                c.wait()
        for s in range(QUARTERS):
            for half in BOTH:
                gather.across(s, half).wait_send()
                keep(s, half).wait()
                if s > 1:
                    gather_y.across(s, half).wait()
                    gather_y.ring(s - 1, half).wait_send()
                if s < AWAY[-1]:
                    gather.ring(s, half).wait_send()


STOPS = (((4, 8), (11, 13), (16, 18)), ((21, 23), (25, 27)))


def gate_up(b, dy, wg, wu, early, tn=256, first=9, second=4):
    (shard, d), n = b.shape, wg.shape[1]
    tokens, J = 8 * shard, n // tn
    quarter, half = tokens // 4, tokens // 2
    phases = ((first, 0, 0, quarter), (J - first, first, 0, half), (second, 0, quarter, half), (second, 0, tokens - quarter, quarter),
              (first - second, second, quarter, tokens - quarter), (J - first, first, half, half))
    tile = lambda rows: pl.BlockSpec((rows, tn), lambda t: (0, _phase(t, phases)))
    outs = ((tokens, n, BF16), (tokens, n, BF16), (tokens, n, BF16), (half, n, F32), (half, n, F32), (tokens, d, BF16), (tokens, d, BF16))
    return pl.pallas_call(
        functools.partial(_gate_up, tn, phases, STOPS),
        grid=(sum(p[0] for p in phases),),
        in_specs=[ANY, ANY, tile(d), tile(d), tile(half)],
        out_specs=[ANY] * len(outs),
        out_shape=[jax.ShapeDtypeStruct((rows, m), w) for rows, m, w in outs],
        scratch_shapes=[pltpu.VMEM((tokens, d), BF16), *(_pair(tokens - quarter, tn, dtype=w) for *_, w in outs[:-2]), *GATHER_SEMS, *GATHER_SEMS,
                        DMA((2,)), DMA((4, 2)), DMA((2, 3, 3))],
        input_output_aliases={1: len(outs) - 1},
        compiler_params=_params(62, 3),
        cost_estimate=_cost(2 * tokens * d * n, wg, wu, wg, wu, wg, wu),
        name="gather_gate_up",
    )(b, dy, wg, wu, early)


def _d_hidden(dy, wd, fu, fg, _, __, dg, du):
    d = nt(dy[...], wd[...]).astype(BF16).astype(F32)
    dg[...] = (d * fg[...]).astype(BF16)
    du[...] = (d * fu[...]).astype(BF16)


def d_hidden(dy, wd, fu, fg, dg, du, tn=256):
    tokens, d = dy.shape
    n, half = wd.shape[0], tokens // 2
    low = pl.BlockSpec((half, tn), lambda i: (1, i))
    return pl.pallas_call(
        _d_hidden,
        grid=(n // tn,),
        in_specs=[pl.BlockSpec((half, d), lambda i: (1, 0), pipeline_mode=pl.Buffered(1)), _down(tn, d), _along(half, tn), _along(half, tn), ANY, ANY],
        out_specs=[low, low],
        out_shape=[jax.ShapeDtypeStruct((tokens, n), BF16)] * 2,
        input_output_aliases={4: 0, 5: 1},
        compiler_params=_params(60),
        cost_estimate=_cost(half * d * n, dy, wd, fu, fg),
        name="d_hidden",
    )(dy, wd, fu, fg, dg, du)


def _da(dq, dkv, wq, wk, wv, out, kv):
    kv[:, :HEAD] = wk[...]
    kv[:, HEAD:] = wv[...]
    out[...] = (nt(dq[...], wq[...]) + nt(dkv[...], kv[...])).astype(BF16)


def d_states(dq, dkv, wq, wk, wv, tn=1024):
    tokens, hq = dq.shape
    d = wq.shape[0]
    whole = lambda t: pl.BlockSpec(t.shape, STILL)
    some = lambda t: _down(tn, t.shape[1])
    return pl.pallas_call(
        _da,
        grid=(d // tn,),
        in_specs=[whole(dq), whole(dkv), some(wq), some(wk), some(wv)],
        out_specs=_along(tokens, tn),
        out_shape=jax.ShapeDtypeStruct((tokens, d), BF16),
        scratch_shapes=[pltpu.VMEM((tn, 2 * HEAD), BF16)],
        compiler_params=_params(56),
        cost_estimate=_cost(dq.size * d, dq, wq, wk, wv),
        name="d_states",
    )(dq, dkv, wq, wk, wv)


class _Task:
    def __init__(self, m, n, widths, ins, outs, A, T, O, in_sem, out_sem):
        self.m, self.n, self.widths = m, n, widths
        self.ins, self.outs, self.A, self.T, self.O, self.in_sem, self.out_sem = ins, outs, A, T, O, in_sem, out_sem

    def left(self, i):
        size = self.A.shape[-1]
        cols = pl.ds(pl.multiple_of(i % self.m * size, size), size)
        return [pltpu.make_async_copy(self.ins[0].at[:, cols], self.A.at[_slot(i)], self.in_sem.at[_slot(i), 0])]

    def right(self, c):
        copies = []
        for k, (t, buf) in enumerate(zip(self.ins[1:], self.T)):
            size = buf.shape[-1]
            copies.append(pltpu.make_async_copy(t.at[:, pl.ds(pl.multiple_of(c * size, size), size)], buf.at[_slot(c)], self.in_sem.at[_slot(c), k + 1]))
        return copies

    def put(self, i):
        copies = []
        for k, (o, buf) in enumerate(zip(self.outs, self.O)):
            rows, cols = (pl.ds(pl.multiple_of(at * size, size), size) for at, size in zip((i % self.m, i // self.m), buf.shape[1:]))
            copies.append(pltpu.make_async_copy(buf.at[_slot(i)], o.at[rows, cols], self.out_sem.at[_slot(i), k]))
        return copies

    def begin(self):
        _start(self.left(0) + self.right(0))

    def run(self, following):
        steps = self.m * self.n

        def step(i, _):
            c = i // self.m

            @pl.when((i == 0) | (self.m > 1))
            def _():
                _wait(self.left(i))

            @pl.when(i % self.m == 0)
            def _():
                _wait(self.right(c))

            @pl.when(i + 1 < steps)
            def _():
                if self.m > 1:
                    _start(self.left(i + 1))
                if self.n > 1:
                    @pl.when((i + 1) % self.m == 0)
                    def _():
                        _start(self.right(c + 1))

            if following is not None:
                @pl.when(i + 1 == steps)
                def _():
                    following.begin()

            @pl.when(i >= 2)
            def _():
                _wait(self.put(i - 2))

            a = self.A[_slot(i) if self.m > 1 else 0]
            outs = iter(self.O)
            for t, widths in zip(self.T, self.widths):
                whole = tt(a, t[_slot(c)]).astype(BF16)
                at = 0
                for w in widths:
                    next(outs)[_slot(i)] = whole[:, at : at + w]
                    at += w
            _start(self.put(i))

        lax.fori_loop(0, steps, step, None)
        for i in range(max(steps - 2, 0), steps):
            _wait(self.put(i))


def _start(copies):
    for c in copies:
        c.start()


def _wait(copies):
    for c in copies:
        c.wait()


def _outer(plan, *refs):
    tasks, refs = [], list(refs)
    take = lambda n: [refs.pop(0) for _ in range(n)]
    ins = [take(1 + len(widths)) for _, _, widths in plan]
    outs = [take(sum(map(len, widths))) for _, _, widths in plan]
    for (m, n, widths), a, o in zip(plan, ins, outs):
        tasks.append(_Task(m, n, widths, a, o, *take(1), take(len(widths)), take(len(o)), *take(2)))
    tasks[0].begin()
    for task, following in zip(tasks, [*tasks[1:], None]):
        task.run(following)


def outer(*tasks, vmem=62):
    ins, out_shape, scratch, plan = [], [], [], []
    for a, ts, tm, tn, *cuts in tasks:
        tokens, rows = a.shape
        tall, wide = [tn or t.shape[1] for t in ts], [t.shape[1] for t in ts]
        plan.append((rows // tm, wide[0] // tall[0], cuts or [(w,) for w in tall]))
        ins += [a, *ts]
        full = [w for widths in (cuts or [(w,) for w in wide]) for w in widths]
        out_shape += [jax.ShapeDtypeStruct((rows, w), BF16) for w in full]
        part = [w for widths in plan[-1][2] for w in widths]
        scratch += [_pair(tokens, tm), *(_pair(tokens, w) for w in tall), *(_pair(tm, w) for w in part),
                    DMA((2, 1 + len(ts))), DMA((2, len(part)))]
    return pl.pallas_call(
        functools.partial(_outer, plan),
        in_specs=[ANY] * len(ins),
        out_specs=[ANY] * len(out_shape),
        out_shape=out_shape,
        scratch_shapes=scratch,
        compiler_params=_params(vmem),
        cost_estimate=_cost(sum(a.size * t.shape[1] for a, ts, *_ in tasks for t in ts), *ins, *out_shape),
        name="outer",
    )(*ins)


def tables(tokens):
    half = HEAD // 2
    angle = np.arange(tokens, dtype=np.float32)[:, None] * np.float32(THETA) ** (-np.arange(half, dtype=np.float32) / np.float32(half))
    cos, sin = np.cos(angle), np.sin(angle)
    return jnp.asarray(np.concatenate([cos, cos], -1)), jnp.asarray(np.concatenate([-sin, sin], -1))


def layer_grads(x, dy, wq, wk, wv, wo, wg, wu, wd):
    cos, sin = tables(8 * x.shape[0])
    q, k, v, a, dy_all, o, lse = qkv(x, dy, wq, wk, wv, cos, sin)
    h, b, early = mm_rs([o], [wo], "nn", False, _after_wo, [x], 2, 2, beside=(dy_all, wd), lag=2)
    hidden, dgate, dup, fu, fg, b, dy_all = gate_up(b, dy_all, wg, wu, early)
    dgate, dup = d_hidden(dy_all, wd, fu, fg, dgate, dup)
    (dh,) = mm_rs([dgate, dup], [wg, wu], "nt", True, _after_norm, [h, dy], 1, 4)
    dh_all = lax.all_gather(dh, "tp", axis=0, tiled=True)
    by_gate, by_up = outer((b, [dgate, dup], 1024, 1792))
    dh_all, by_gate, by_up = lax.optimization_barrier((dh_all, by_gate, by_up))
    d_o = nt(dh_all, wo).astype(BF16)
    dq, dkv = attend_bwd(q, k, v, d_o, o, lse, cos, sin)
    da = lax.psum_scatter(d_states(dq, dkv, wq, wk, wv), "tp", scatter_dimension=0, tiled=True)
    by_down, by_o, by_q, by_k, by_v = outer(
        (hidden, [dy_all], 1792, 1024), (o, [dh_all], 1024, 1024), (a, [dq, dkv], 1024, None, (dq.shape[1],), (HEAD, HEAD)))
    return finish(x, dh, da), by_q, by_k, by_v, by_o, by_gate, by_up, by_down


def solution(mesh):
    def step(x, dy, *weights):
        by_x, *by_w = layer_grads(x[0], dy[0], *weights)
        return (by_x[None], *by_w)

    states, by_columns, by_rows = P("dp", "tp", None), P(None, "tp"), P("tp", None)
    weights = (by_columns, by_columns, by_columns, by_rows, by_columns, by_columns, by_rows)
    own = tuple(P("dp", "tp") if spec == by_columns else P(("dp", "tp"), None) for spec in weights)
    return jax.shard_map(step, mesh=mesh, in_specs=(states, states, *weights), out_specs=(states, *own), check_vma=False)
```

```python
import functools

import jax
import jax.numpy as jnp
import numpy as np
from jax import lax
from jax.experimental import pallas as pl
from jax.experimental.pallas import tpu as pltpu
from jax.sharding import PartitionSpec as P

HEAD = 128
THETA = 10000
SHARD = 128
PART = SHARD // 2
PAIR = 2 * SHARD
MESH = pl.DeviceIdType.MESH
DMA = pltpu.SemaphoreType.DMA
F32, BF16 = jnp.float32, jnp.bfloat16
ANY = pl.BlockSpec(memory_space=pl.ANY)
EPS = 1e-6
MIB = 2**20
BOTH, AWAY, QUARTERS = range(2), range(1, 4), 4
STILL = lambda *_: (0, 0)
NEG = -1e30
HIDDEN = 2 * NEG
LOG2E = 1.4426950408889634


def _contract(ca, cb):
    return lambda a, b: lax.dot_general(a, b, (((ca,), (cb,)), ((), ())), preferred_element_type=F32)


nn, nt, tt = _contract(1, 0), _contract(1, 1), _contract(0, 0)


def _slot(i):
    return i % 2


def _pair(*shape, dtype=BF16):
    return pltpu.VMEM((2, *shape), dtype)


def _params(vmem, cid=None, **more):
    if cid is not None:
        more |= {"collective_id": cid, "has_side_effects": True}
    return pltpu.CompilerParams(vmem_limit_bytes=vmem * MIB, **more)


def _down(rows, columns):
    return pl.BlockSpec((rows, columns), lambda i: (i, 0))


def _along(rows, columns):
    return pl.BlockSpec((rows, columns), lambda i: (0, i))


def _cost(products, *arrays):
    return pl.CostEstimate(flops=products + products, transcendentals=0, bytes_accessed=sum(t.size * t.dtype.itemsize for t in arrays))


def _hidden(first_key, first_query, bk, bq):
    keys = lax.broadcasted_iota(jnp.int32, (bk, bq), 0) + first_key
    return keys > lax.broadcasted_iota(jnp.int32, (bk, bq), 1) + first_query


def _head(n):
    return slice(n * HEAD, (n + 1) * HEAD)


def _blocks(block, iq, n):
    lax.fori_loop(0, iq * n, lambda j, _: block(j, False), None)
    lax.fori_loop(iq * n, (iq + 1) * n, lambda j, _: block(j, True), None)


def _attend(q, k, v, o, lse, top_s, mix_s, iq, bk):
    bq, heads = top_s.shape[1], top_s.shape[0]
    scale = HEAD**-0.5
    e = scale * LOG2E
    rows = pl.ds(pl.multiple_of(iq * bq, bq), bq)
    top_s[...] = jnp.full(top_s.shape, NEG, F32)
    mix_s[...] = jnp.zeros(mix_s.shape, F32)
    ones = jnp.ones((mix_s.shape[1] - HEAD, bk), BF16)

    def block(j, masked):
        here = pl.ds(pl.multiple_of(j * bk, bk), bk)
        scores = [nt(k[here, :], q[rows, _head(n)]) for n in range(heads)]
        hide = _hidden(j * bk, iq * bq, bk, bq) if masked else None
        weights, keeps = [], []
        for n, s in enumerate(scores):
            if masked:
                s = jnp.where(hide, HIDDEN, s)
            old = top_s[n : n + 1, :]
            top = jnp.maximum(old, s.max(axis=0, keepdims=True))
            top_s[n : n + 1, :] = top
            weights.append(jnp.exp2((s - top) * e).astype(BF16))
            keeps.append(jnp.exp2((old - top) * e))
        values = jnp.concatenate([v[here, :].T, ones], axis=0)
        for n in range(heads):
            mix_s[n] = mix_s[n] * keeps[n] + nn(values, weights[n])

    _blocks(block, iq, bq // bk)
    for n in range(heads):
        total = mix_s[n, HEAD : HEAD + 1, :]
        o[rows, _head(n)] = (mix_s[n, :HEAD, :] * (1 / total)).T.astype(BF16)
        lse[n : n + 1, rows] = top_s[n : n + 1, :] * scale + jnp.log(total)


def _unturned(t, c, n):
    t = t.astype(BF16).astype(F32)
    return (t * c - pltpu.roll(t, HEAD // 2, 1) * n).astype(BF16)


def _attend_bwd(q_ref, k_ref, v_ref, do_ref, o_ref, lse_ref, cos_ref, sin_ref, cosk_ref, sink_ref, dq_ref, dkv_ref, dq_s, dk_s, dv_s, delta_s, *, bk):
    bq, heads = q_ref.shape[0], q_ref.shape[1] // HEAD
    iq = pl.program_id(0)
    scale = HEAD**-0.5
    e = scale * LOG2E

    @pl.when(iq == 0)
    def _():
        dk_s[...] = jnp.zeros_like(dk_s)
        dv_s[...] = jnp.zeros_like(dv_s)

    dq_s[...] = jnp.zeros_like(dq_s)
    for n in range(heads):
        both = do_ref[:, _head(n)].astype(F32) * o_ref[:, _head(n)].astype(F32)
        delta_s[n : n + 1, :] = both.T.sum(axis=0, keepdims=True)

    def block(j, masked):
        here = pl.ds(pl.multiple_of(j * bk, bk), bk)
        scores = [nt(k_ref[here, :], q_ref[:, _head(n)]) for n in range(heads)]
        dps = [nt(v_ref[here, :], do_ref[:, _head(n)]) for n in range(heads)]
        hide = _hidden(j * bk, iq * bq, bk, bq) if masked else None
        for n in range(heads):
            p = jnp.exp2(scores[n] * e - lse_ref[n : n + 1, :] * LOG2E)
            if masked:
                p = jnp.where(hide, 0.0, p)
            ds = (p * (dps[n] - delta_s[n : n + 1, :])).astype(BF16)
            dv_s[here, :] += nn(p.astype(BF16), do_ref[:, _head(n)])
            dk_s[here, :] += nn(ds, q_ref[:, _head(n)])
            dq_s[n] += nn(k_ref[here, :].T, ds)

    _blocks(block, iq, bq // bk)
    for n in range(heads):
        dq_ref[:, _head(n)] = _unturned((dq_s[n] * scale).T, cos_ref[...], sin_ref[...])

    @pl.when(iq == pl.num_programs(0) - 1)
    def _():
        dkv_ref[:, :HEAD] = _unturned(dk_s[...] * scale, cosk_ref[...], sink_ref[...])
        dkv_ref[:, HEAD:] = dv_s[...].astype(BF16)


def attend_bwd(q, k, v, d_o, o, lse, cos, sin, bq=256, bk=256):
    tokens, d = q.shape
    heads = d // HEAD
    rows = _down(bq, d)
    some, every = _down(bq, HEAD), pl.BlockSpec((tokens, HEAD), STILL)
    return pl.pallas_call(
        functools.partial(_attend_bwd, bk=bk),
        grid=(tokens // bq,),
        in_specs=[rows, every, every, rows, rows, _along(heads, bq), some, some, every, every],
        out_specs=[rows, pl.BlockSpec((tokens, 2 * HEAD), STILL)],
        out_shape=[jax.ShapeDtypeStruct((tokens, d), BF16), jax.ShapeDtypeStruct((tokens, 2 * HEAD), BF16)],
        scratch_shapes=[pltpu.VMEM((heads, HEAD, bq), F32), pltpu.VMEM((tokens, HEAD), F32), pltpu.VMEM((tokens, HEAD), F32), pltpu.VMEM((heads, bq), F32)],
        compiler_params=_params(56),
        cost_estimate=_cost(5 * tokens * tokens * d, q, d_o, o, q),
        name="attend_bwd",
    )(q, k, v, d_o, o, lse, cos, sin, cos, sin)


def _flip(c):
    return c + (c // 2) * (1 - 2 * (_slot(c)))


def _place():
    me = lax.axis_index("tp")
    core, pos = me % 2, _flip(me // 2)
    turn = 1 - 2 * core
    at = lambda k, c: _flip((pos + turn * k + 8) % 4) * 2 + c
    return core, at, me + turn, at(1, core), at(-1, core)


def _owner(at, core, s, side):
    return at(-s if side == 0 else s, core if side == 0 else 1 - core)


def _greet(devices):
    barrier = pltpu.get_barrier_semaphore()
    for d in devices:
        pl.semaphore_signal(barrier, inc=1, device_id={"tp": d}, device_id_type=MESH)
    pl.semaphore_wait(barrier, len(devices))


def _send(src, dst, ssem, rsem, dev):
    return pltpu.make_async_remote_copy(src_ref=src, dst_ref=dst, send_sem=ssem, recv_sem=rsem, device_id={"tp": dev}, device_id_type=MESH)


def _place_of(s, half, side):
    return ((s * 2 + half) * 2 + side) * PART


class _Gather:
    def __init__(self, ref, sems, nxt, partner):
        self.ref, self.sems, self.nxt, self.partner = ref, sems, nxt, partner

    def part(self, s, half, side):
        return self.ref.at[pl.ds(pl.multiple_of(_place_of(s, half, side), PART), PART)]

    def ring(self, s, half, src=None):
        rs, rr, _, _ = self.sems
        return _send(self.part(s, half, 0) if src is None else src, self.part(s + 1, half, 0), rs.at[s, half], rr.at[s + 1, half], self.nxt)

    def across(self, s, half, src=None):
        _, _, xs, xr = self.sems
        return _send(self.part(s, half, 0) if src is None else src, self.part(s, half, 1), xs.at[s, half], xr.at[s, half], self.partner)


GATHER_SEMS = [DMA((4, 2))] * 4


def _norm_rows(src, dst, at_row, rows, step=16):
    def body(i, _):
        r = pl.multiple_of(i * step, step)
        wide = src[pl.ds(r, step), :].astype(F32)
        scale = lax.rsqrt(jnp.mean(wide * wide, -1, keepdims=True) + EPS)
        dst[pl.ds(pl.multiple_of(at_row(r), step), step), :] = (wide * scale).astype(BF16)

    lax.fori_loop(rows[0] // step, rows[1] // step, body, None)


def _qkv(x, dy, wq, wk, wv, cos, sin, q_out, k_out, v_out, a_out, y_out, o, lse, xb, yb, A, W, cosb, sinb, O, top_s, mix_s,
         rs, rr, xs, xr, ys, yr, zs, zr, lsem, osem, asem, bk):
    core, at, partner, nxt, prv = _place()
    gather = _Gather(A, (rs, rr, xs, xr), nxt, partner)
    gather_y = _Gather(y_out, (ys, yr, zs, zr), nxt, partner)
    hq = wq.shape[1]
    hk = wk.shape[1]
    cuts = (pl.ds(0, hq), pl.ds(hq, hk), pl.ds(hq + hk, hk))
    moves = ((x, xb), (cos, cosb), (sin, sinb), *((w, W.at[:, c]) for w, c in zip((wq, wk, wv), cuts)), (dy, yb))
    loads = [pltpu.make_async_copy(a, b, lsem.at[i]) for i, (a, b) in enumerate(moves)]
    loads[0].start()
    _greet((partner, nxt, prv))
    loads[0].wait()
    own = [yb.at[pl.ds(half * PART, PART)] for half in BOTH]
    keep_y = [pltpu.make_async_copy(own[half], gather_y.part(0, half, 0), asem.at[QUARTERS, half, 0]) for half in BOTH]
    for half in BOTH:
        _norm_rows(xb, A, lambda r: r + half * PART, (half * PART, half * PART + PART))
        gather.ring(0, half).start()
        gather.across(0, half).start()
    _start(loads[1:])
    _wait(loads[1:])
    for half in BOTH:
        keep_y[half].start()
        gather_y.across(0, half, own[half]).start()

    def there(s, half, side):
        return pl.ds(pl.multiple_of(_owner(at, core, s, side) * SHARD + half * PART, PART), PART)

    def keep(s, half, side):
        return pltpu.make_async_copy(gather.part(s, half, side), a_out.at[there(s, half, side)], asem.at[s, half, side])

    def unit(u, _):
        s, half = u // 2, u % 2

        @pl.when(s > 0)
        def _():
            gather.ring(s - 1, half).wait_recv()

            @pl.when(s < AWAY[-1])
            def _():
                gather.ring(s, half).start()

            gather.across(s, half).start()

        @pl.when(s == AWAY[-1])
        def _():
            gather_y.ring(0, half, yb.at[pl.ds(pl.multiple_of(half * PART, PART), PART)]).start()

        gather.across(s, half).wait_recv()
        keep(s, half, 0).start()
        keep(s, half, 1).start()
        rows = A[pl.ds(pl.multiple_of(u * SHARD, SHARD), SHARD), :]
        out = nn(rows, W[...]).astype(BF16)
        for side in BOTH:
            to = there(s, half, side)
            c, n = cosb[to, :], sinb[to, :]
            mine = out[side * PART : (side + 1) * PART, :]
            for i in range((hq + hk) // HEAD):
                t = mine[:, _head(i)].astype(F32)
                O[to, _head(i)] = (t * c + pltpu.roll(t, HEAD // 2, 1) * n).astype(BF16)
            O[to, hq + hk :] = mine[:, hq + hk :]

    lax.fori_loop(0, QUARTERS * len(BOTH), unit, None)
    puts = [pltpu.make_async_copy(O.at[:, c], t, osem.at[i]) for i, (c, t) in enumerate(zip(cuts, (q_out, k_out, v_out)))]
    for c in puts:
        c.start()
    q, k, v = (O.at[:, c] for c in cuts)

    def rows(iq, _):
        _attend(q, k, v, o, lse, top_s, mix_s, iq, bk)
        gather_y.ring(0, iq).wait_recv()
        gather_y.across(1, iq).start()

    lax.fori_loop(0, len(BOTH), rows, None)
    for c in puts + keep_y:
        c.wait()
    for half in BOTH:
        gather_y.ring(0, half, own[half]).wait_send()
        for s in range(QUARTERS):
            gather.across(s, half).wait_send()
            if s < AWAY[-1]:
                gather.ring(s, half).wait_send()
            if s < len(BOTH):
                gather_y.across(s, half, None if s else own[half]).wait()
            for side in BOTH:
                keep(s, half, side).wait()


def qkv(x, dy, wq, wk, wv, cos, sin, bk=256):
    d, hq, hk, tokens = x.shape[1], wq.shape[1], wk.shape[1], cos.shape[0]
    heads, bq = hq // HEAD, tokens // len(BOTH)
    vmem = pl.BlockSpec(memory_space=pltpu.VMEM)
    return pl.pallas_call(
        functools.partial(_qkv, bk=bk),
        in_specs=[ANY] * 7,
        out_specs=[ANY] * 5 + [vmem] * 2,
        out_shape=[jax.ShapeDtypeStruct((tokens, n), BF16) for n in (hq, hk, hk, d, d, hq)] + [jax.ShapeDtypeStruct((heads, tokens), F32)],
        scratch_shapes=[pltpu.VMEM(x.shape, BF16), pltpu.VMEM(x.shape, BF16), pltpu.VMEM((tokens, d), BF16), pltpu.VMEM((d, hq + 2 * hk), BF16),
                        pltpu.VMEM(cos.shape, F32), pltpu.VMEM(sin.shape, F32), pltpu.VMEM((tokens, hq + 2 * hk), BF16),
                        pltpu.VMEM((heads, bq), F32), pltpu.VMEM((heads, HEAD + 8, bq), F32),
                        *GATHER_SEMS, *GATHER_SEMS, DMA((7,)), DMA((3,)), DMA((5, 2, 2))],
        compiler_params=_params(62, 1),
        cost_estimate=_cost(tokens * d * hq, x, dy, wq, wk, wv),
        name="gather_qkv",
    )(x, dy, wq, wk, wv, cos, sin)


def _mm_rs(nl, form, arrived, J, tn, lag, after, extra, beside, *refs):
    lhs, rhs, refs = refs[:nl], refs[nl:2 * nl], refs[2 * nl:]
    left, right, refs = (*refs[:2], refs[2:]) if beside else (None, None, refs)
    ins, outs, refs = refs[:extra[0]], refs[extra[0]:sum(extra)], refs[sum(extra):]
    product, refs = (refs[0], refs[1:]) if beside else (None, refs)
    L, refs = refs[:nl], refs[nl:]
    got, refs = refs[:extra[0]], refs[extra[0]:]
    give, refs = refs[:extra[1]], refs[extra[1]:]
    fin, P_, SD, RD, SR, RR, lsem, esem, sd_sem, rd_sem, sr_sem, rr_sem = refs
    g = pl.program_id(0)
    last, slots, waits = J + 3 * lag, 3 * lag + 2, lag + 1
    core, at, partner, nxt, prv = _place()

    def to_partner(j):
        return _send(SD.at[_slot(j)], RD.at[j % 4], sd_sem.at[_slot(j)], rd_sem.at[j % 4], partner)

    def to_next(k, j):
        return _send(SR.at[j % waits, k], RR.at[j, k], sr_sem.at[j % waits, k], rr_sem.at[j, k], nxt)

    def half_of(side):
        terms = ((nt if form == "nt" else nn)(l[pl.ds(side * 4 * SHARD, 4 * SHARD), :], r[...]) for l, r in zip(L, rhs))
        return functools.reduce(jnp.add, terms).reshape(4, SHARD, tn)

    def loads(side):
        copies = []
        for i in range(nl):
            for s in range(4):
                for half in BOTH:
                    row = _place_of(s, half, side) if arrived else _owner(at, core, s, side) * SHARD + half * PART
                    copies.append(pltpu.make_async_copy(lhs[i].at[pl.ds(pl.multiple_of(row, PART), PART)],
                                                        L[i].at[pl.ds((side * 4 + s) * SHARD + half * PART, PART)], lsem.at[i, side, s, half]))
        return copies

    extras = [pltpu.make_async_copy(a, b, esem.at[i]) for i, (a, b) in enumerate(zip(ins, got))]

    @pl.when(g == 0)
    def _():
        for side in (1, 0):
            for c in loads(side):
                c.start()
        for c in extras:
            c.start()
        _greet((partner, nxt, prv))
        for c in loads(1):
            c.wait()

    @pl.when(g < J)
    def _():
        SD[_slot(g)] = half_of(1).astype(BF16)
        to_partner(g).start()

    @pl.when(g == 0)
    def _():
        for c in loads(0):
            c.wait()

    @pl.when((g >= 1) & (g <= J))
    def _():
        j = g - 1
        to_partner(j).wait()
        SR[j % waits, 0] = (P_[j % slots, 1] + RD[j % 4, 1].astype(F32)).astype(BF16)
        to_next(0, j).start()
        for s in (0, 2, 3):
            P_[j % slots, s] += RD[j % 4, s].astype(F32)

    for k, slot in enumerate((2, 3, 0)):
        at_step = 1 + lag * (k + 1)

        @pl.when((g >= at_step) & (g < J + at_step))
        def _():
            j = g - at_step
            to_next(k, j).wait()
            total = P_[j % slots, slot] + RR[j, k].astype(F32)
            if slot:
                SR[j % waits, k + 1] = total.astype(BF16)
                to_next(k + 1, j).start()
            else:
                fin[:, pl.ds(pl.multiple_of(j * tn, tn), tn)] = total

    @pl.when(g < J)
    def _():
        P_[g % slots] = half_of(0)

    if beside:
        later = (last - beside) * 2 // 3

        @pl.when((g >= later) & (g < later + beside))
        def _():
            product[...] = nt(left[...], right[...]).astype(BF16)

    @pl.when(g == last)
    def _():
        for c in extras:
            c.wait()
        after(fin, got, give)
        for i, (a, b) in enumerate(zip(give, outs)):
            pltpu.make_async_copy(a, b, esem.at[i]).start()
        for i, (a, b) in enumerate(zip(give, outs)):
            pltpu.make_async_copy(a, b, esem.at[i]).wait()


def mm_rs(lhs, rhs, form, arrived, after, ins, outs, cid, beside=(), lag=1, tn=512, few=256, vmem=62):
    nl = len(lhs)
    n = rhs[0].shape[1] if form == "nn" else rhs[0].shape[0]
    J = n // tn
    tile = lambda g: jnp.minimum(g, J - 1)
    if form == "nn":
        rspec = [pl.BlockSpec((r.shape[0], tn), lambda g: (0, tile(g))) for r in rhs]
    else:
        rspec = [pl.BlockSpec((tn, r.shape[1]), lambda g: (tile(g), 0)) for r in rhs]
    steps, bspec, pspec, pshape = 0, [], [], []
    if beside:
        left, right = beside
        steps, rows = right.shape[0] // few, left.shape[0] // 2
        part = lambda g: jnp.clip(g - (J + 3 * lag - steps) * 2 // 3, 0, steps - 1)
        bspec = [pl.BlockSpec((rows, left.shape[1]), STILL, pipeline_mode=pl.Buffered(1)), pl.BlockSpec((few, right.shape[1]), lambda g: (part(g), 0))]
        pspec = [pl.BlockSpec((rows, few), lambda g: (0, part(g)))]
        pshape = [jax.ShapeDtypeStruct((rows, right.shape[0]), BF16)]
    return pl.pallas_call(
        functools.partial(_mm_rs, nl, form, arrived, J, tn, lag, after, (len(ins), outs), steps),
        grid=(J + 3 * lag + 1,),
        in_specs=[ANY] * nl + rspec + bspec + [ANY] * len(ins),
        out_specs=[ANY] * outs + pspec,
        out_shape=[jax.ShapeDtypeStruct((SHARD, n), BF16)] * outs + pshape,
        scratch_shapes=[pltpu.VMEM(l.shape, l.dtype) for l in lhs] + [pltpu.VMEM((SHARD, n), BF16)] * (len(ins) + outs) + [
            pltpu.VMEM((SHARD, n), F32),
            pltpu.VMEM((3 * lag + 2, 4, SHARD, tn), F32), _pair(4, SHARD, tn), pltpu.VMEM((4, 4, SHARD, tn), BF16),
            pltpu.VMEM((lag + 1, 3, SHARD, tn), BF16), pltpu.VMEM((J, 3, SHARD, tn), BF16),
            DMA((nl, 2, 4, 2)), DMA((max(len(ins), outs),)), DMA((2,)), DMA((4,)), DMA((lag + 1, 3)), DMA((J, 3))],
        compiler_params=_params(vmem, cid),
        cost_estimate=_cost(sum(l.size for l in lhs) * n, *lhs, *rhs),
        name="mm_rs",
    )(*lhs, *rhs, *beside, *ins)


def _after_wo(total, ins, outs):
    (x,), (h, b) = ins, outs

    def body(i, _):
        r = pl.ds(pl.multiple_of(i * 16, 16), 16)
        new = (x[r, :].astype(F32) + total[r, :].astype(BF16).astype(F32)).astype(BF16)
        h[r, :] = new
        wide = new.astype(F32)
        b[r, :] = (wide * lax.rsqrt(jnp.mean(wide * wide, -1, keepdims=True) + EPS)).astype(BF16)

    lax.fori_loop(0, SHARD // 16, body, None)


def _norm_back(wide, ct):
    scale = lax.rsqrt(jnp.mean(wide * wide, -1, keepdims=True) + EPS)
    along = jnp.mean(ct * wide, -1, keepdims=True)
    return ct * scale - wide * (scale * scale * scale * along)


def _after_norm(total, ins, outs):
    (h, dy), (dh,) = ins, outs

    def body(i, _):
        r = pl.ds(pl.multiple_of(i * 16, 16), 16)
        back = _norm_back(h[r, :].astype(F32), total[r, :].astype(BF16).astype(F32))
        dh[r, :] = (dy[r, :].astype(F32) + back.astype(BF16).astype(F32)).astype(BF16)

    lax.fori_loop(0, SHARD // 16, body, None)


def _finish(x, dh, da, dx):
    back = _norm_back(x[...].astype(F32), da[...].astype(F32))
    dx[...] = (dh[...].astype(F32) + back.astype(BF16).astype(F32)).astype(BF16)


def finish(x, dh, da, rows=64):
    some = _down(rows, x.shape[1])
    return pl.pallas_call(_finish, grid=(x.shape[0] // rows,), in_specs=[some] * 3, out_specs=some, out_shape=jax.ShapeDtypeStruct(x.shape, BF16),
                          compiler_params=_params(56), cost_estimate=_cost(x.size, x, x, x, x), name="finish")(x, dh, da)


def _phase(t, phases):
    at, tile = 0, 0
    for n, first, *_ in phases:
        tile = jnp.where(t >= at, t - at + first, tile)
        at += n
    return tile


def _gate_up(tn, phases, stops, b, dy, wg, wu, early, hid_out, dg_out, du_out, fu_out, fg_out, b_out, dy_out, B, WG, WU, hid, dg, du, fu, fg, rs, rr, xs, xr, ys, yr, zs, zr, lsem, bsem, osem, wsem):
    t = pl.program_id(0)
    core, at, partner, nxt, prv = _place()
    gather = _Gather(B, (rs, rr, xs, xr), nxt, partner)
    gather_y = _Gather(dy_out, (ys, yr, zs, zr), nxt, partner)
    own = [pl.ds(half * PART, PART) for half in BOTH]
    load = [pltpu.make_async_copy(b.at[own[half]], gather.part(0, half, 0), lsem.at[half]) for half in BOTH]
    keep = lambda s, half: pltpu.make_async_copy(B.at[pl.ds(_place_of(s, half, 0), SHARD)], b_out.at[pl.ds(_place_of(s, half, 0), SHARD)], bsem.at[s, half])

    def weights(u):
        cols = pl.ds(pl.multiple_of(_phase(u, phases) * tn, tn), tn)
        return [pltpu.make_async_copy(w.at[:, cols], buf.at[_slot(u)], wsem.at[_slot(u), i]) for i, (w, buf) in enumerate(((wg, WG), (wu, WU)))]

    def whole(s):
        for half in BOTH:
            gather.across(s, half).wait_recv()
            keep(s, half).start()

    @pl.when(t == 0)
    def _():
        for c in load:
            c.start()
        _greet((partner, nxt, prv))
        for half in BOTH:
            load[half].wait()
            gather.ring(0, half).start()
            gather.across(0, half).start()
        _start(weights(0))
        whole(0)

    @pl.when(t + 1 < sum(p[0] for p in phases))
    def _():
        _start(weights(t + 1))

    _wait(weights(t))

    for s in AWAY:
        for half in BOTH:
            @pl.when(t == stops[0][s - 1][half])
            def _():
                gather.ring(s - 1, half).wait_recv()
                if s < AWAY[-1]:
                    gather.ring(s, half).start()
                gather.across(s, half).start()
                if s == AWAY[1] and half:
                    for h in BOTH:
                        gather_y.ring(1, h).start()

            if s > 1:
                @pl.when(t == stops[1][s - 2][half])
                def _():
                    gather_y.ring(s - 1, half).wait_recv()
                    if s < AWAY[-1]:
                        gather_y.ring(s, half).start()
                    gather_y.across(s, half).start()

    slot = t % 2

    half = fu_out.shape[0]

    def put(u, row, size):
        cols = pl.ds(pl.multiple_of(_phase(u, phases) * tn, tn), tn)
        copies = []
        for c, m in enumerate(range(0, size, PAIR)):
            r = row + m
            late = r >= half
            to = ((hid, hid_out, r), (fu, fu_out, r - half), (fg, fg_out, r - half)) if late else ((hid, hid_out, r), (du, du_out, r), (dg, dg_out, r))
            copies += [pltpu.make_async_copy(v.at[_slot(u), pl.ds(m, PAIR)], o.at[pl.ds(at, PAIR), cols], osem.at[_slot(u), c, i]) for i, (v, o, at) in enumerate(to)]
        return copies

    start, ready = 0, 1
    for n, _, row, size in phases:
        @pl.when((t >= start + 2) & (t < start + n + 2))
        def _():
            for c in put(t - 2, row, size):
                c.wait()

        while ready * PAIR < row + size:
            @pl.when(t == start)
            def _():
                whole(ready)

            ready += 1

        @pl.when((t >= start) & (t < start + n))
        def _():
            for m in range(0, size, PAIR):
                rows = B[pl.ds(row + m, PAIR), :]
                gate = nn(rows, WG[slot])
                up = nn(rows, WU[slot])
                sig = jax.nn.sigmoid(gate)
                act = gate * sig
                to = pl.ds(m, PAIR)
                hid[slot, to, :] = (act * up).astype(BF16)
                slope = up * (sig * (1 + gate * (1 - sig)))
                if row + m < half:
                    d = early[pl.ds(row + m, PAIR), :].astype(F32)
                    du[slot, to, :] = (d * act).astype(BF16)
                    dg[slot, to, :] = (d * slope).astype(BF16)
                else:
                    fu[slot, to, :] = act
                    fg[slot, to, :] = slope
            for c in put(t, row, size):
                c.start()

        start += n

    @pl.when(t == start - 1)
    def _():
        for u in (start - 2, start - 1):
            for c in put(u, *phases[-1][2:]):
                c.wait()
        for s in range(QUARTERS):
            for half in BOTH:
                gather.across(s, half).wait_send()
                keep(s, half).wait()
                if s > 1:
                    gather_y.across(s, half).wait()
                    gather_y.ring(s - 1, half).wait_send()
                if s < AWAY[-1]:
                    gather.ring(s, half).wait_send()


STOPS = (((4, 7), (10, 12), (15, 17)), ((20, 22), (24, 26)))


def gate_up(b, dy, wg, wu, early, tn=256, first=8, second=3):
    (shard, d), n = b.shape, wg.shape[1]
    tokens, J = 8 * shard, n // tn
    quarter, half = tokens // 4, tokens // 2
    phases = ((first, 0, 0, quarter), (J - first, first, 0, half), (second, 0, quarter, half), (second, 0, tokens - quarter, quarter),
              (first - second, second, quarter, tokens - quarter), (J - first, first, half, half))
    tile = lambda rows: pl.BlockSpec((rows, tn), lambda t: (0, _phase(t, phases)))
    outs = ((tokens, n, BF16), (tokens, n, BF16), (tokens, n, BF16), (half, n, F32), (half, n, F32), (tokens, d, BF16), (tokens, d, BF16))
    return pl.pallas_call(
        functools.partial(_gate_up, tn, phases, STOPS),
        grid=(sum(p[0] for p in phases),),
        in_specs=[ANY] * 4 + [tile(half)],
        out_specs=[ANY] * len(outs),
        out_shape=[jax.ShapeDtypeStruct((rows, m), w) for rows, m, w in outs],
        scratch_shapes=[pltpu.VMEM((tokens, d), BF16), _pair(d, tn), _pair(d, tn), *(_pair(tokens - quarter, tn, dtype=w) for *_, w in outs[:-2]), *GATHER_SEMS, *GATHER_SEMS,
                        DMA((2,)), DMA((4, 2)), DMA((2, 3, 3)), DMA((2, 2))],
        input_output_aliases={1: len(outs) - 1},
        compiler_params=_params(62, 3),
        cost_estimate=_cost(2 * tokens * d * n, wg, wu, wg, wu, wg, wu),
        name="gather_gate_up",
    )(b, dy, wg, wu, early)


def _d_hidden(dy, wd, fu, fg, _, __, dg, du):
    d = nt(dy[...], wd[...]).astype(BF16).astype(F32)
    dg[...] = (d * fg[...]).astype(BF16)
    du[...] = (d * fu[...]).astype(BF16)


def d_hidden(dy, wd, fu, fg, dg, du, tn=256):
    tokens, d = dy.shape
    n, half = wd.shape[0], tokens // 2
    low = pl.BlockSpec((half, tn), lambda i: (1, i))
    return pl.pallas_call(
        _d_hidden,
        grid=(n // tn,),
        in_specs=[pl.BlockSpec((half, d), lambda i: (1, 0), pipeline_mode=pl.Buffered(1)), _down(tn, d), _along(half, tn), _along(half, tn), ANY, ANY],
        out_specs=[low, low],
        out_shape=[jax.ShapeDtypeStruct((tokens, n), BF16)] * 2,
        input_output_aliases={4: 0, 5: 1},
        compiler_params=_params(60),
        cost_estimate=_cost(half * d * n, dy, wd, fu, fg),
        name="d_hidden",
    )(dy, wd, fu, fg, dg, du)


def _da(dq, dkv, wq, wk, wv, out, kv):
    kv[:, :HEAD] = wk[...]
    kv[:, HEAD:] = wv[...]
    out[...] = (nt(dq[...], wq[...]) + nt(dkv[...], kv[...])).astype(BF16)


def d_states(dq, dkv, wq, wk, wv, tn=1024):
    tokens, hq = dq.shape
    d = wq.shape[0]
    whole = lambda t: pl.BlockSpec(t.shape, STILL)
    some = lambda t: _down(tn, t.shape[1])
    return pl.pallas_call(
        _da,
        grid=(d // tn,),
        in_specs=[whole(dq), whole(dkv), some(wq), some(wk), some(wv)],
        out_specs=_along(tokens, tn),
        out_shape=jax.ShapeDtypeStruct((tokens, d), BF16),
        scratch_shapes=[pltpu.VMEM((tn, 2 * HEAD), BF16)],
        compiler_params=_params(56),
        cost_estimate=_cost(dq.size * d, dq, wq, wk, wv),
        name="d_states",
    )(dq, dkv, wq, wk, wv)


class _Task:
    def __init__(self, m, n, widths, ins, outs, A, T, O, in_sem, out_sem):
        self.m, self.n, self.widths = m, n, widths
        self.ins, self.outs, self.A, self.T, self.O, self.in_sem, self.out_sem = ins, outs, A, T, O, in_sem, out_sem

    def left(self, i):
        size = self.A.shape[-1]
        cols = pl.ds(pl.multiple_of(i % self.m * size, size), size)
        return [pltpu.make_async_copy(self.ins[0].at[:, cols], self.A.at[_slot(i)], self.in_sem.at[_slot(i), 0])]

    def right(self, c):
        copies = []
        for k, (t, buf) in enumerate(zip(self.ins[1:], self.T)):
            size = buf.shape[-1]
            copies.append(pltpu.make_async_copy(t.at[:, pl.ds(pl.multiple_of(c * size, size), size)], buf.at[_slot(c)], self.in_sem.at[_slot(c), k + 1]))
        return copies

    def put(self, i):
        copies = []
        for k, (o, buf) in enumerate(zip(self.outs, self.O)):
            rows, cols = (pl.ds(pl.multiple_of(at * size, size), size) for at, size in zip((i % self.m, i // self.m), buf.shape[1:]))
            copies.append(pltpu.make_async_copy(buf.at[_slot(i)], o.at[rows, cols], self.out_sem.at[_slot(i), k]))
        return copies

    def begin(self):
        _start(self.left(0) + self.right(0))

    def run(self, following):
        steps = self.m * self.n

        def step(i, _):
            c = i // self.m

            @pl.when((i == 0) | (self.m > 1))
            def _():
                _wait(self.left(i))

            @pl.when(i % self.m == 0)
            def _():
                _wait(self.right(c))

            @pl.when(i + 1 < steps)
            def _():
                if self.m > 1:
                    _start(self.left(i + 1))
                if self.n > 1:
                    @pl.when((i + 1) % self.m == 0)
                    def _():
                        _start(self.right(c + 1))

            if following is not None:
                @pl.when(i + 1 == steps)
                def _():
                    following.begin()

            @pl.when(i >= 2)
            def _():
                _wait(self.put(i - 2))

            a = self.A[_slot(i) if self.m > 1 else 0]
            outs = iter(self.O)
            for t, widths in zip(self.T, self.widths):
                whole = tt(a, t[_slot(c)]).astype(BF16)
                at = 0
                for w in widths:
                    next(outs)[_slot(i)] = whole[:, at : at + w]
                    at += w
            _start(self.put(i))

        lax.fori_loop(0, steps, step, None)
        for i in range(max(steps - 2, 0), steps):
            _wait(self.put(i))


def _start(copies):
    for c in copies:
        c.start()


def _wait(copies):
    for c in copies:
        c.wait()


def _outer(plan, *refs):
    tasks, refs = [], list(refs)
    take = lambda n: [refs.pop(0) for _ in range(n)]
    ins = [take(1 + len(widths)) for _, _, widths in plan]
    outs = [take(sum(map(len, widths))) for _, _, widths in plan]
    for (m, n, widths), a, o in zip(plan, ins, outs):
        tasks.append(_Task(m, n, widths, a, o, *take(1), take(len(widths)), take(len(o)), *take(2)))
    tasks[0].begin()
    for task, following in zip(tasks, [*tasks[1:], None]):
        task.run(following)


def outer(*tasks, vmem=62):
    ins, out_shape, scratch, plan = [], [], [], []
    for a, ts, tm, tn, *cuts in tasks:
        tokens, rows = a.shape
        tall, wide = [tn or t.shape[1] for t in ts], [t.shape[1] for t in ts]
        plan.append((rows // tm, wide[0] // tall[0], cuts or [(w,) for w in tall]))
        ins += [a, *ts]
        full = [w for widths in (cuts or [(w,) for w in wide]) for w in widths]
        out_shape += [jax.ShapeDtypeStruct((rows, w), BF16) for w in full]
        part = [w for widths in plan[-1][2] for w in widths]
        scratch += [_pair(tokens, tm), *(_pair(tokens, w) for w in tall), *(_pair(tm, w) for w in part),
                    DMA((2, 1 + len(ts))), DMA((2, len(part)))]
    return pl.pallas_call(
        functools.partial(_outer, plan),
        in_specs=[ANY] * len(ins),
        out_specs=[ANY] * len(out_shape),
        out_shape=out_shape,
        scratch_shapes=scratch,
        compiler_params=_params(vmem),
        cost_estimate=_cost(sum(a.size * t.shape[1] for a, ts, *_ in tasks for t in ts), *ins, *out_shape),
        name="outer",
    )(*ins)


def tables(tokens):
    half = HEAD // 2
    angle = np.arange(tokens, dtype=np.float32)[:, None] * np.float32(THETA) ** (-np.arange(half, dtype=np.float32) / np.float32(half))
    cos, sin = np.cos(angle), np.sin(angle)
    return jnp.asarray(np.concatenate([cos, cos], -1)), jnp.asarray(np.concatenate([-sin, sin], -1))


def layer_grads(x, dy, wq, wk, wv, wo, wg, wu, wd):
    cos, sin = tables(8 * x.shape[0])
    q, k, v, a, dy_all, o, lse = qkv(x, dy, wq, wk, wv, cos, sin)
    h, b, early = mm_rs([o], [wo], "nn", False, _after_wo, [x], 2, 2, beside=(dy_all, wd), lag=2)
    hidden, dgate, dup, fu, fg, b, dy_all = gate_up(b, dy_all, wg, wu, early)
    dgate, dup = d_hidden(dy_all, wd, fu, fg, dgate, dup)
    (dh,) = mm_rs([dgate, dup], [wg, wu], "nt", True, _after_norm, [h, dy], 1, 4)
    dh_all = lax.all_gather(dh, "tp", axis=0, tiled=True)
    by_gate, by_up = outer((b, [dgate, dup], 1024, 1792))
    dh_all, by_gate, by_up = lax.optimization_barrier((dh_all, by_gate, by_up))
    d_o = nt(dh_all, wo).astype(BF16)
    dq, dkv = attend_bwd(q, k, v, d_o, o, lse, cos, sin)
    da = lax.psum_scatter(d_states(dq, dkv, wq, wk, wv), "tp", scatter_dimension=0, tiled=True)
    by_down, by_o, by_q, by_k, by_v = outer(
        (hidden, [dy_all], 1792, 1024), (o, [dh_all], 1024, 1024), (a, [dq, dkv], 1024, None, (dq.shape[1],), (HEAD, HEAD)))
    return finish(x, dh, da), by_q, by_k, by_v, by_o, by_gate, by_up, by_down


def solution(mesh):
    def step(x, dy, *weights):
        by_x, *by_w = layer_grads(x[0], dy[0], *weights)
        return (by_x[None], *by_w)

    states, by_columns, by_rows = P("dp", "tp", None), P(None, "tp"), P("tp", None)
    weights = (by_columns, by_columns, by_columns, by_rows, by_columns, by_columns, by_rows)
    own = tuple(P("dp", "tp") if spec == by_columns else P(("dp", "tp"), None) for spec in weights)
    return jax.shard_map(step, mesh=mesh, in_specs=(states, states, *weights), out_specs=(states, *own), check_vma=False)
```
